8 devices in a mesh: data: 1 (over z), row: 2 (over y), col: 4 (over x, core).
Axes of the slice: x: 2, y: 2, z: 1, core: 2. Of those that a mesh axis runs over, the one named last changes fastest.
Arguments:
- tokens: bfloat16 [1536, 2048], P(('data', 'row', 'col'))
- expert_ids: int32 [1536, 8], P(('data', 'row', 'col'))
- gate_weights: float32 [1536, 8], P(('data', 'row', 'col'))
- w_in: bfloat16 [64, 2048, 1024], P(('row', 'col'))
- w_out: bfloat16 [64, 1024, 2048], P(('row', 'col'))
Outputs:
- output: bfloat16 [1536, 2048], P(('data', 'row', 'col'))
All inputs are finite; a program needn't handle non-finite values.
Results may differ from the reference program's by a relative error of at most 0.00449034.
Values are sent between devices in bfloat16 or wider.
A program may use at most 1 GiB of HBM per device.

```python
import jax
import jax.numpy as jnp
from jax import lax

D = 2048
FF = 1024
EXPERTS = 64
TOP = 8
TOK_DEV = 192
ROW = 2
COL = 4
GROUP = ROW * COL
TOKENS = GROUP * TOK_DEV
CAP = TOKENS * TOP // EXPERTS
AVG_LOAD = TOK_DEV * TOP // EXPERTS


def draw_routing(base_key):
    key_split, key_device = jax.random.split(base_key)
    shuffled = jax.random.permutation(key_split, EXPERTS)
    hot_set = shuffled[: EXPERTS // 2]
    cold_set = shuffled[EXPERTS // 2:]

    def one_device(device_index):
        device_key = jax.random.fold_in(key_device, device_index)
        key_shift, key_order, key_rows = jax.random.split(device_key, 3)
        shift_by = jax.random.randint(key_shift, (EXPERTS // 2,), 0, AVG_LOAD + 1)
        shift_by = shift_by.at[0].set(AVG_LOAD)
        counts = jnp.zeros((EXPERTS,), jnp.int32)
        counts = counts.at[hot_set].set(AVG_LOAD + shift_by).at[cold_set].set(AVG_LOAD - shift_by)
        expert_order = jax.random.permutation(key_order, EXPERTS)
        run_end = jnp.cumsum(counts[expert_order])
        position = jnp.arange(TOK_DEV * TOP)
        run_index = jnp.searchsorted(run_end, position, side='right')
        id_table = expert_order[run_index].reshape(TOP, TOK_DEV).T
        row_order = jax.random.permutation(key_rows, TOK_DEV)
        return id_table[row_order]

    return lax.map(one_device, jnp.arange(GROUP)).reshape(TOKENS, TOP).astype(jnp.int32)


def setup_inputs(seed: int = 0, part: int = 0) -> dict:
    base_key = jax.random.key(seed)
    key_tok, key_ids, key_gate, key_in, key_out = jax.random.split(base_key, 5)
    tokens = jax.random.normal(jax.random.fold_in(key_tok, part), (TOKENS, D), jnp.float32)
    expert_ids = draw_routing(jax.random.fold_in(key_ids, part))
    gate_weights = jax.random.uniform(jax.random.fold_in(key_gate, part), (TOKENS, TOP), jnp.float32, 0.25, 1.25) * TOP ** -0.5
    w_in = jax.random.normal(key_in, (EXPERTS, D, FF), jnp.float32) * D ** -0.5
    w_out = jax.random.normal(key_out, (EXPERTS, FF, D), jnp.float32) * FF ** -0.5
    return {'tokens': tokens.astype(jnp.bfloat16), 'expert_ids': expert_ids, 'gate_weights': gate_weights, 'w_in': w_in.astype(jnp.bfloat16), 'w_out': w_out.astype(jnp.bfloat16)}


def reference(tokens, expert_ids, gate_weights, w_in, w_out):
    flat_ids = expert_ids.reshape(-1)
    pair_count = flat_ids.shape[0]
    sort_order = jnp.argsort(flat_ids, stable=True)
    counts = jnp.bincount(flat_ids, length=EXPERTS)
    starts = jnp.cumsum(counts) - counts
    sorted_rank = jnp.arange(pair_count) - starts[flat_ids[sort_order]]
    pair_rank = jnp.zeros((pair_count,), jnp.int32).at[sort_order].set(sorted_rank)
    slot_of_pair = jnp.where(pair_rank < CAP, flat_ids * CAP + pair_rank, EXPERTS * CAP)
    token_of_pair = jnp.arange(pair_count) // TOP
    slot_token = jnp.full((EXPERTS * CAP,), TOKENS, jnp.int32).at[slot_of_pair].set(token_of_pair, mode='drop')
    padded = jnp.concatenate([tokens, jnp.zeros((1, D), tokens.dtype)], axis=0)

    def expert_ffn(operands):
        rows_index, w_first, w_second = operands
        buffer = padded[rows_index]
        hidden = jax.nn.gelu(jnp.dot(buffer, w_first, preferred_element_type=jnp.float32)).astype(jnp.bfloat16)
        return jnp.dot(hidden, w_second, preferred_element_type=jnp.float32).astype(jnp.bfloat16)

    expert_out = lax.map(expert_ffn, (slot_token.reshape(EXPERTS, CAP), w_in, w_out))
    out_pad = jnp.concatenate([expert_out.reshape(EXPERTS * CAP, D), jnp.zeros((1, D), expert_out.dtype)], axis=0)

    def combine(operands):
        block_tok, block_slot, block_gate = operands
        gathered = out_pad[block_slot]
        weighted = jnp.einsum('tk,tkd->td', block_gate.astype(jnp.float32), gathered.astype(jnp.float32))
        return (block_tok.astype(jnp.float32) + weighted).astype(jnp.bfloat16)

    layer_out = lax.map(combine, (tokens.reshape(GROUP, TOK_DEV, D), slot_of_pair.reshape(GROUP, TOK_DEV, TOP), gate_weights.reshape(GROUP, TOK_DEV, TOP)))
    return layer_out.reshape(TOKENS, D)
```

```python
import functools

import jax
import jax.numpy as jnp
from jax import lax
from jax.experimental import pallas as pl
from jax.experimental.pallas import tpu as pltpu
from jax.sharding import PartitionSpec as P

GRID_AXES = ('row', 'col')
MESH = pl.DeviceIdType.MESH
BF = jnp.bfloat16
F32 = jnp.float32
NI = 12
NO = 12
WIN = 64
DIRECT = (1, 2, 4, 6)
REMOTE = (2, 4, 6)


def moe_kernel(cfg, ids_ref, gate_ref, tok_hbm, wi_hbm, wo_hbm, out_ref,
               ids_all, gate_all, tok_all, pmat, cmat, hacc, hbf, wi, wo, obuf, d2d_in, ici_out, ici_in, own,
               slot_buf, zbuf, start_v, start_s,
               tok_sem, wi_sem, wo_sem, ms_sem, mr_sem, gs_sem, gr_sem, as_sem, ar_sem, ds_sem, dr_sem, is_sem, ir_sem, st_sem):
    tok_dev, cap, nexp, nch, wd, ff = cfg
    ntok = 8 * tok_dev
    i = lax.axis_index('row')
    j = lax.axis_index('col')
    j_flip = j + 1 - 2 * lax.rem(j, 2)

    def rel(r):
        jj = j_flip if r & 1 else j
        if r & 2:
            jj = lax.rem(jj + 2, 4)
        ii = lax.rem(i + 1, 2) if r & 4 else i
        return ii, jj

    def dev(r):
        ii, jj = rel(r)
        return {'row': ii, 'col': jj}

    def gidx(r):
        ii, jj = rel(r)
        return ii * 4 + jj

    def rows_of(r):
        return pl.ds(pl.multiple_of(gidx(r) * tok_dev, 64), tok_dev)

    me = gidx(0)

    def tok_copy(c):
        return pltpu.make_async_copy(tok_hbm.at[:, pl.ds(c * wd, wd)], tok_all.at[c, rows_of(0), :], tok_sem.at[c])

    def wi_copy(s):
        c, e = s // nexp, lax.rem(s, nexp)
        slot = lax.rem(s, NI)
        return pltpu.make_async_copy(wi_hbm.at[e, pl.ds(pl.multiple_of(c * wd, wd), wd), :], wi.at[slot], wi_sem.at[slot])

    def wo_copy(s):
        c, e = s // nexp, lax.rem(s, nexp)
        slot = lax.rem(s, NO)
        return pltpu.make_async_copy(wo_hbm.at[e, :, pl.ds(pl.multiple_of(c * wd, wd), wd)], wo.at[slot], wo_sem.at[slot])

    for c in range(nch):
        tok_copy(c).start()

    def prefetch_i(s, _):
        wi_copy(s).start()
        return 0

    def prefetch_o(s, _):
        wo_copy(s).start()
        return 0

    lax.fori_loop(0, NI, prefetch_i, 0)
    lax.fori_loop(0, NO, prefetch_o, 0)
    ids_all[me] = ids_ref[...]
    gate_all[me] = gate_ref[...]

    bar = pltpu.get_barrier_semaphore()
    for r in range(1, 8):
        pl.semaphore_signal(bar, inc=1, device_id=dev(r), device_id_type=MESH)
    pl.semaphore_wait(bar, 7)

    def ids_copy(r):
        return pltpu.make_async_remote_copy(ids_ref, ids_all.at[me], ms_sem.at[r - 1], mr_sem.at[r - 1],
                                            device_id=dev(r), device_id_type=MESH)

    def gate_copy(r):
        return pltpu.make_async_remote_copy(gate_ref, gate_all.at[me], gs_sem.at[r - 1], gr_sem.at[r - 1],
                                            device_id=dev(r), device_id_type=MESH)

    def ag_copy(c, r, origin, to):
        ref = tok_all.at[c, rows_of(origin), :]
        return pltpu.make_async_remote_copy(ref, ref, as_sem.at[c, r - 1], ar_sem.at[c, r - 1],
                                            device_id=dev(to), device_id_type=MESH)

    for r in range(1, 8):
        ids_copy(r).start()
        gate_copy(r).start()
    for c in range(nch):
        tok_copy(c).wait()
        for r in DIRECT:
            ag_copy(c, r, 0, r).start()

    for r in range(1, 8):
        ids_copy(r).wait_recv()
        gate_copy(r).wait_recv()

    lane = lax.broadcasted_iota(jnp.int32, (8, 128), 1)

    def compact(ref):
        out = []
        for m in range(4):
            a = ref[2 * m]
            b = pltpu.roll(ref[2 * m + 1], 64, 1)
            out += [a[:, :128], jnp.where(lane < 64, a[:, 128:], b[:, :128]), b[:, 128:]]
        return out

    id_blocks, gate_blocks = compact(ids_all), compact(gate_all)
    eid = lax.broadcasted_iota(jnp.int32, (8, 128), 0) + me * nexp
    imasks, gates = [], []
    for idb, gb in zip(id_blocks, gate_blocks):
        m = jnp.zeros((8, 128), jnp.int32)
        g = jnp.zeros((8, 128), F32)
        for k in range(8):
            hit = idb[k:k + 1, :] == eid
            m = jnp.where(hit, 1, m)
            g = jnp.where(hit, gb[k:k + 1, :], g)
        imasks.append(m)
        gates.append(g)
    masks = [m.astype(F32) for m in imasks]
    nb = len(masks)
    tri = jnp.where(lax.broadcasted_iota(jnp.int32, (128, 128), 0) < lax.broadcasted_iota(jnp.int32, (128, 128), 1),
                    1.0, 0.0).astype(BF)
    cums = jnp.dot(jnp.concatenate(masks, axis=0).astype(BF), tri, preferred_element_type=F32)
    carry = jnp.zeros((8, 1), F32)
    ranks = []
    for b in range(nb):
        ranks.append(cums[b * 8:b * 8 + 8, :] + carry)
        carry = carry + jnp.sum(masks[b], axis=1, keepdims=True)
    starts, seen = [], jnp.zeros((8, 128), jnp.int32)
    table = jnp.zeros((8, 128), jnp.int32)
    for g in range(8):
        b = 3 * (g // 2) + g % 2
        before = seen + jnp.where(lane < 64, imasks[b], 0) if g % 2 else seen
        off = jnp.sum(before, axis=1, keepdims=True)
        start16 = jnp.minimum(off >> 4, (cap - WIN) // 16)
        table = jnp.where(lane == g, start16, table)
        starts.append((start16 * 16).astype(F32))
        seen = seen + imasks[b]
        if g % 2:
            seen = seen + imasks[b + 1]
    start_v[...] = table
    st = pltpu.make_async_copy(start_v, start_s, st_sem)
    st.start()
    for b in range(nb):
        m = b // 3
        if b % 3 == 0:
            start = starts[2 * m]
        elif b % 3 == 1:
            start = jnp.where(lane < 64, starts[2 * m], starts[2 * m + 1])
        else:
            start = starts[2 * m + 1]
        keep = (masks[b] > 0.0) & (ranks[b] < float(cap))
        slot_buf[:, b * 128:(b + 1) * 128] = jnp.where(keep, ranks[b], -1.0)
        g1 = gates[b].astype(BF).astype(F32)
        rem1 = gates[b] - g1
        g2 = rem1.astype(BF).astype(F32)
        g3 = rem1 - g2
        zbuf[b, 0:8, :] = jnp.where(keep, ranks[b] - start, -1.0)
        zbuf[b, 8:16, :] = g1
        zbuf[b, 16:24, :] = g2
        zbuf[b, 24:32, :] = g3

    def build_p(e, _):
        row = slot_buf[pl.ds(e, 1), :]
        pos = lax.broadcasted_iota(jnp.int32, (cap, ntok), 0).astype(F32)
        pmat[pl.ds(pl.multiple_of(e * cap, 64), cap), :] = jnp.where(pos == row, 1.0, 0.0).astype(BF)
        return 0

    lax.fori_loop(0, nexp, build_p, 0)
    nwin = nexp * WIN

    def build_c(b, _):
        z = jnp.concatenate([zbuf[b], jnp.zeros((96, 128), F32)], axis=0)
        zt = jnp.transpose(z).astype(BF)
        ex = jnp.where(lax.broadcasted_iota(jnp.int32, (128, 4 * nwin), 0)
                       == lax.broadcasted_iota(jnp.int32, (128, 4 * nwin), 1) // WIN, 1.0, 0.0).astype(BF)
        y = jnp.dot(zt, ex, preferred_element_type=F32)
        wpos = lax.rem(lax.broadcasted_iota(jnp.int32, (128, nwin), 1), WIN).astype(F32)
        hit = y[:, :nwin] == wpos
        rows = pl.ds(pl.multiple_of(b * 128, 128), 128)
        for k in range(3):
            cmat[k, rows, :] = jnp.where(hit, y[:, (k + 1) * nwin:(k + 2) * nwin], 0.0).astype(BF)
        return 0

    lax.fori_loop(0, nb, build_c, 0)

    def first(c, last):
        for r in DIRECT:
            ag_copy(c, r, 0, r).wait_recv()
            if r in REMOTE:
                ag_copy(c, r + 1, r, 1).start()
        for r in REMOTE:
            ag_copy(c, r + 1, 0, 1).wait_recv()

        def pair(q, _):
            for h in range(2):
                e = q * 2 + h
                s = c * nexp + e
                slot = lax.rem(s, NI)
                wi_copy(s).wait()
                bufr = jnp.dot(pmat[pl.ds(pl.multiple_of(e * cap, 64), cap), :], tok_all[c],
                               preferred_element_type=F32).astype(BF)
                for n in range(2):
                    y = jnp.dot(bufr, wi[slot, :, n * (ff // 2):(n + 1) * (ff // 2)], preferred_element_type=F32)
                    if c > 0:
                        y = y + hacc[e * 2 + n]
                    if last:
                        hbf[pl.ds(pl.multiple_of(e * cap, 64), cap), n * (ff // 2):(n + 1) * (ff // 2)] = (
                            jax.nn.gelu(y, approximate=True).astype(BF))
                    else:
                        hacc[e * 2 + n] = y

                @pl.when(s + NI < nch * nexp)
                def _():
                    wi_copy(s + NI).start()
            return 0

        lax.fori_loop(0, nexp // 2, pair, 0)

    for c in range(nch):
        first(c, c == nch - 1)
    st.wait()

    def d2d_copy(c, q):
        k = c * 4 + q
        return pltpu.make_async_remote_copy(hacc.at[k], d2d_in.at[k], ds_sem.at[k], dr_sem.at[k],
                                            device_id=dev(1), device_id_type=MESH)

    def ici_copy(c, q):
        k = c * 3 + q
        return pltpu.make_async_remote_copy(ici_out.at[k], ici_in.at[k], is_sem.at[k], ir_sem.at[k],
                                            device_id=dev(REMOTE[q]), device_id_type=MESH)

    def combine(r):
        g = gidx(r)
        parts = []
        for e in range(nexp):
            at = e * (cap // 16) + start_s[e, g]
            parts.append(obuf[pl.ds(at, WIN // 16)].reshape(WIN, wd))
        win = jnp.concatenate(parts, axis=0)
        rows = pl.ds(pl.multiple_of(g * tok_dev, 64), tok_dev)
        lhs = jnp.concatenate([cmat[k, rows, :] for k in range(3)], axis=0)
        y = jnp.dot(lhs, win, preferred_element_type=F32)
        return y[:tok_dev] + y[tok_dev:2 * tok_dev] + y[2 * tok_dev:]

    def second(c, _):
        def pair(q, _):
            for h in range(2):
                e = q * 2 + h
                s = c * nexp + e
                slot = lax.rem(s, NO)
                wo_copy(s).wait()
                rows = pl.ds(pl.multiple_of(e * cap, 64), cap)
                y = jnp.dot(hbf[rows, :], wo[slot], preferred_element_type=F32).astype(BF)
                obuf[pl.ds(e * (cap // 16), cap // 16)] = y.reshape(cap // 16, 16, wd)

                @pl.when(s + NO < nch * nexp)
                def _():
                    wo_copy(s + NO).start()
            return 0

        lax.fori_loop(0, nexp // 2, pair, 0)
        for q, r in enumerate((2, 4, 6, 0)):
            hacc[c * 4 + q] = combine(r + 1)
            d2d_copy(c, q).start()
        for q, r in enumerate((2, 4, 6, 0)):
            y = combine(r)
            d2d_copy(c, q).wait_recv()
            y = y + d2d_in[c * 4 + q]
            if r:
                ici_out[c * 3 + q] = y.astype(BF)
                ici_copy(c, q).start()
            else:
                own[c] = y
        return 0

    lax.fori_loop(0, nch, second, 0)

    for c in range(nch):
        y = tok_all[c, rows_of(0), :].astype(F32) + own[c]
        for q in range(3):
            ici_copy(c, q).wait_recv()
            y = y + ici_in[c * 3 + q].astype(F32)
        out_ref[:, c * wd:(c + 1) * wd] = y.astype(BF)

    for r in range(1, 8):
        ids_copy(r).wait_send()
        gate_copy(r).wait_send()
    for c in range(nch):
        for r in DIRECT:
            ag_copy(c, r, 0, r).wait_send()
        for r in REMOTE:
            ag_copy(c, r + 1, r, 1).wait_send()
        for q in range(4):
            d2d_copy(c, q).wait_send()
        for q in range(3):
            ici_copy(c, q).wait_send()


def solution(mesh):
    group_size = mesh.shape['row'] * mesh.shape['col']

    def device_fn(tokens, expert_ids, gate_weights, w_in, w_out):
        tok_dev, width = tokens.shape
        top_k = expert_ids.shape[1]
        nexp, _, ff = w_in.shape
        cap = tok_dev * group_size * top_k // (nexp * group_size)
        ntok = tok_dev * group_size
        nch = 4
        wd = width // nch
        ids = jnp.pad(expert_ids.T, ((0, 0), (0, 256 - tok_dev)), constant_values=-1)
        gates = jnp.pad(gate_weights.T, ((0, 0), (0, 256 - tok_dev)))
        dma = pltpu.SemaphoreType.DMA
        cfg = (tok_dev, cap, nexp, nch, wd, ff)
        vm = pl.BlockSpec(memory_space=pltpu.VMEM)
        hb = pl.BlockSpec(memory_space=pl.ANY)
        return pl.pallas_call(
            functools.partial(moe_kernel, cfg),
            out_shape=jax.ShapeDtypeStruct((tok_dev, width), BF),
            in_specs=[vm, vm, hb, hb, hb],
            out_specs=vm,
            scratch_shapes=[
                pltpu.VMEM((8, 8, 256), jnp.int32),
                pltpu.VMEM((8, 8, 256), F32),
                pltpu.VMEM((nch, ntok, wd), BF),
                pltpu.VMEM((nexp * cap, ntok), BF),
                pltpu.VMEM((3, ntok, nexp * WIN), BF),
                pltpu.VMEM((nexp * 2, cap, ff // 2), F32),
                pltpu.VMEM((nexp * cap, ff), BF),
                pltpu.VMEM((NI, wd, ff), BF),
                pltpu.VMEM((NO, ff, wd), BF),
                pltpu.VMEM((nexp * cap // 16, 16, wd), BF),
                pltpu.VMEM((nch * 4, tok_dev, wd), F32),
                pltpu.VMEM((nch * 3, tok_dev, wd), BF),
                pltpu.VMEM((nch * 3, tok_dev, wd), BF),
                pltpu.VMEM((nch, tok_dev, wd), F32),
                pltpu.VMEM((8, ntok), F32),
                pltpu.VMEM((ntok // 128, 32, 128), F32),
                pltpu.VMEM((8, 128), jnp.int32),
                pltpu.SMEM((8, 128), jnp.int32),
                dma((nch,)), dma((NI,)), dma((NO,)), dma((7,)), dma((7,)), dma((7,)), dma((7,)), dma((nch, 7)), dma((nch, 7)),
                dma((nch * 4,)), dma((nch * 4,)), dma((nch * 3,)), dma((nch * 3,)), dma,
            ],
            compiler_params=pltpu.CompilerParams(collective_id=0, has_side_effects=True, vmem_limit_bytes=67000000),
        )(ids, gates, tokens, w_in, w_out)

    token_spec = P(('data', 'row', 'col'), None)
    expert_spec = P(GRID_AXES, None, None)
    return jax.shard_map(device_fn, mesh=mesh, in_specs=(token_spec, token_spec, token_spec, expert_spec, expert_spec),
                         out_specs=token_spec, check_vma=False)
```

```python
import functools

import jax
import jax.numpy as jnp
from jax import lax
from jax.experimental import pallas as pl
from jax.experimental.pallas import tpu as pltpu
from jax.sharding import PartitionSpec as P

GRID_AXES = ('row', 'col')
MESH = pl.DeviceIdType.MESH
BF = jnp.bfloat16
F32 = jnp.float32
NI = 20
NO = 20
WIN = 64
LEAD = 2
AG_KINDS = ((0, None, 1), (0, None, 2), (0, None, 4), (2, 0, 4), (4, 1, 2), (2, None, 1), (4, None, 1), (6, 0, 1), (6, 1, 1))
RETURN_ORDER = (6, 2, 4, 0)


def moe_kernel(cfg, ids_ref, gate_ref, tok_hbm, wi_hbm, wo_hbm, out_hbm,
               ids_all, gate_all, tok_all, pmat, cmat, hacc, hbf, wi, wo, obuf, d2d_in, out1, in1, out2, in2, kept, own, outv,
               slot_buf, zbuf, start_v, start_s,
               tok_sem, wi_sem, wo_sem, ms_sem, mr_sem, gs_sem, gr_sem, as_sem, ar_sem, ds_sem, dr_sem,
               s1_sem, r1_sem, s2_sem, r2_sem, st_sem, out_sem):
    tok_dev, cap, nexp, nch, wd, ff = cfg
    ntok = 8 * tok_dev
    half = tok_dev // 2
    i = lax.axis_index('row')
    j = lax.axis_index('col')
    j_flip = j + 1 - 2 * lax.rem(j, 2)

    def rel(r):
        jj = j_flip if r & 1 else j
        if r & 2:
            jj = lax.rem(jj + 2, 4)
        ii = lax.rem(i + 1, 2) if r & 4 else i
        return ii, jj

    def dev(r):
        ii, jj = rel(r)
        return {'row': ii, 'col': jj}

    def gidx(r):
        ii, jj = rel(r)
        return ii * 4 + jj

    def rows_of(r):
        return pl.ds(pl.multiple_of(gidx(r) * tok_dev, 64), tok_dev)

    me = gidx(0)

    def tok_copy(c):
        return pltpu.make_async_copy(tok_hbm.at[:, pl.ds(c * wd, wd)], tok_all.at[c, rows_of(0), :], tok_sem.at[c])

    def wi_copy(s):
        c, e = s // nexp, lax.rem(s, nexp)
        slot = lax.rem(s, NI)
        return pltpu.make_async_copy(wi_hbm.at[e, pl.ds(pl.multiple_of(c * wd, wd), wd), :], wi.at[slot], wi_sem.at[slot])

    def wo_copy(s):
        c, e = s // nexp, lax.rem(s, nexp)
        slot = lax.rem(s, NO)
        return pltpu.make_async_copy(wo_hbm.at[e, :, pl.ds(pl.multiple_of(c * wd, wd), wd)], wo.at[slot], wo_sem.at[slot])

    def out_copy(c):
        return pltpu.make_async_copy(outv.at[c], out_hbm.at[:, pl.ds(pl.multiple_of(c * wd, wd), wd)], out_sem.at[c])

    for c in range(nch):
        tok_copy(c).start()

    def prefetch_i(s, _):
        wi_copy(s).start()
        return 0

    def prefetch_o(s, _):
        wo_copy(s).start()
        return 0

    lax.fori_loop(0, NI, prefetch_i, 0)
    lax.fori_loop(0, NO, prefetch_o, 0)
    ids_all[me] = jnp.zeros((8, 256), jnp.int32)
    ids_all[me, :, :tok_dev] = ids_ref[...]
    gate_all[me] = jnp.zeros((8, 256), F32)
    gate_all[me, :, :tok_dev] = gate_ref[...]

    bar = pltpu.get_barrier_semaphore()
    for r in range(1, 8):
        pl.semaphore_signal(bar, inc=1, device_id=dev(r), device_id_type=MESH)
    pl.semaphore_wait(bar, 7)

    def ids_copy(r):
        return pltpu.make_async_remote_copy(ids_all.at[me], ids_all.at[me], ms_sem.at[r - 1], mr_sem.at[r - 1],
                                            device_id=dev(r), device_id_type=MESH)

    def gate_copy(r):
        return pltpu.make_async_remote_copy(gate_all.at[me], gate_all.at[me], gs_sem.at[r - 1], gr_sem.at[r - 1],
                                            device_id=dev(r), device_id_type=MESH)

    def ag_copy(c, kind, mine):
        owner, part, to = AG_KINDS[kind]
        if not mine:
            owner = owner ^ to
        start, size = gidx(owner) * tok_dev, tok_dev
        if part is not None:
            start, size = start + part * half, half
        ref = tok_all.at[c, pl.ds(pl.multiple_of(start, 32), size), :]
        return pltpu.make_async_remote_copy(ref, ref, as_sem.at[c, kind], ar_sem.at[c, kind],
                                            device_id=dev(to), device_id_type=MESH)

    def send_own(c):
        tok_copy(c).wait()
        for kind in (1, 2, 0):
            ag_copy(c, kind, True).start()

    def near(c):
        ag_copy(c, 1, False).wait_recv()
        ag_copy(c, 3, True).start()
        ag_copy(c, 5, True).start()
        ag_copy(c, 2, False).wait_recv()
        ag_copy(c, 4, True).start()
        ag_copy(c, 6, True).start()

    def far(c):
        ag_copy(c, 3, False).wait_recv()
        ag_copy(c, 7, True).start()
        ag_copy(c, 4, False).wait_recv()
        ag_copy(c, 8, True).start()

    for r in range(1, 8):
        ids_copy(r).start()
        gate_copy(r).start()
    for c in range(LEAD):
        send_own(c)

    for r in range(1, 8):
        ids_copy(r).wait_recv()
        gate_copy(r).wait_recv()

    lane = lax.broadcasted_iota(jnp.int32, (8, 128), 1)

    def compact(ref):
        out = []
        for m in range(4):
            a = ref[2 * m]
            b = pltpu.roll(ref[2 * m + 1], 64, 1)
            out += [a[:, :128], jnp.where(lane < 64, a[:, 128:], b[:, :128]), b[:, 128:]]
        return out

    id_blocks, gate_blocks = compact(ids_all), compact(gate_all)
    eid = lax.broadcasted_iota(jnp.int32, (8, 128), 0) + me * nexp
    imasks, gates = [], []
    for idb, gb in zip(id_blocks, gate_blocks):
        m = jnp.zeros((8, 128), jnp.int32)
        g = jnp.zeros((8, 128), F32)
        for k in range(8):
            hit = idb[k:k + 1, :] == eid
            m = jnp.where(hit, 1, m)
            g = jnp.where(hit, gb[k:k + 1, :], g)
        imasks.append(m)
        gates.append(g)
    masks = [m.astype(F32) for m in imasks]
    nb = len(masks)
    tri = jnp.where(lax.broadcasted_iota(jnp.int32, (128, 128), 0) < lax.broadcasted_iota(jnp.int32, (128, 128), 1),
                    1.0, 0.0).astype(BF)
    cums = jnp.dot(jnp.concatenate(masks, axis=0).astype(BF), tri, preferred_element_type=F32)
    carry = jnp.zeros((8, 1), F32)
    ranks = []
    for b in range(nb):
        ranks.append(cums[b * 8:b * 8 + 8, :] + carry)
        carry = carry + jnp.sum(masks[b], axis=1, keepdims=True)
    starts, seen = [], jnp.zeros((8, 128), jnp.int32)
    table = jnp.zeros((8, 128), jnp.int32)
    for g in range(8):
        b = 3 * (g // 2) + g % 2
        before = seen + jnp.where(lane < 64, imasks[b], 0) if g % 2 else seen
        off = jnp.sum(before, axis=1, keepdims=True)
        start16 = jnp.minimum(off >> 4, (cap - WIN) // 16)
        table = jnp.where(lane == g, start16, table)
        starts.append((start16 * 16).astype(F32))
        seen = seen + imasks[b]
        if g % 2:
            seen = seen + imasks[b + 1]
    start_v[...] = table
    st = pltpu.make_async_copy(start_v, start_s, st_sem)
    st.start()
    for b in range(nb):
        m = b // 3
        if b % 3 == 0:
            start = starts[2 * m]
        elif b % 3 == 1:
            start = jnp.where(lane < 64, starts[2 * m], starts[2 * m + 1])
        else:
            start = starts[2 * m + 1]
        keep = (masks[b] > 0.0) & (ranks[b] < float(cap))
        slot_buf[:, b * 128:(b + 1) * 128] = jnp.where(keep, ranks[b], -1.0)
        g1 = gates[b].astype(BF).astype(F32)
        rem1 = gates[b] - g1
        g2 = rem1.astype(BF).astype(F32)
        g3 = rem1 - g2
        zbuf[b, 0:8, :] = jnp.where(keep, ranks[b] - start, -1.0)
        zbuf[b, 8:16, :] = g1
        zbuf[b, 16:24, :] = g2
        zbuf[b, 24:32, :] = g3

    def build_p(e, _):
        row = slot_buf[pl.ds(e, 1), :]
        pos = lax.broadcasted_iota(jnp.int32, (cap, ntok), 0).astype(F32)
        pmat[pl.ds(pl.multiple_of(e * cap, 64), cap), :] = jnp.where(pos == row, 1.0, 0.0).astype(BF)
        return 0

    nwin = nexp * WIN

    def build_c(b, _):
        z = jnp.concatenate([zbuf[b], jnp.zeros((96, 128), F32)], axis=0)
        zt = jnp.transpose(z).astype(BF)
        ex = jnp.where(lax.broadcasted_iota(jnp.int32, (128, 4 * nwin), 0)
                       == lax.broadcasted_iota(jnp.int32, (128, 4 * nwin), 1) // WIN, 1.0, 0.0).astype(BF)
        y = jnp.dot(zt, ex, preferred_element_type=F32)
        wpos = lax.rem(lax.broadcasted_iota(jnp.int32, (128, nwin), 1), WIN).astype(F32)
        hit = y[:, :nwin] == wpos
        rows = pl.ds(pl.multiple_of(b * 128, 128), 128)
        for k in range(3):
            cmat[k, rows, :] = jnp.where(hit, y[:, (k + 1) * nwin:(k + 2) * nwin], 0.0).astype(BF)
        return 0

    def zero(k, _):
        hacc[k] = jnp.zeros((cap, wd), F32)
        return 0

    def first(c, last):
        for kind in (0, 5, 6, 7, 8):
            ag_copy(c, kind, False).wait_recv()

        def pair(q, _):
            for h in range(2):
                e = q * 2 + h
                s = c * nexp + e
                slot = lax.rem(s, NI)
                rows = pl.ds(pl.multiple_of(e * cap, 64), cap)
                wi_copy(s).wait()
                bufr = jnp.dot(pmat[rows, :], tok_all[c], preferred_element_type=F32).astype(BF)
                y = jnp.dot(bufr, wi[slot], preferred_element_type=F32)
                for n in range(ff // wd):
                    yn = y[:, n * wd:(n + 1) * wd] + hacc[e * (ff // wd) + n]
                    if last:
                        hbf[rows, n * wd:(n + 1) * wd] = jax.nn.gelu(yn, approximate=True).astype(BF)
                    else:
                        hacc[e * (ff // wd) + n] = yn

                @pl.when(s + NI < nch * nexp)
                def _():
                    wi_copy(s + NI).start()
            return 0

        lax.fori_loop(0, nexp // 2, pair, 0)

    near(0)
    send_own(LEAD)
    lax.fori_loop(0, nexp, build_p, 0)
    lax.fori_loop(0, nexp * ff // wd, zero, 0)
    near(1)
    send_own(LEAD + 1)
    lax.fori_loop(0, nb, build_c, 0)
    far(0)

    def step(c, _):
        @pl.when(c < nch)
        def _():
            near(c)

        @pl.when(c + LEAD < nch)
        def _():
            send_own(c + LEAD)
        first(c - 2, False)
        far(c - 1)
        return 0

    lax.fori_loop(2, nch + 1, step, 0)
    first(nch - 1, True)
    st.wait()

    def d2d_copy(c, q):
        k = c * 4 + q
        return pltpu.make_async_remote_copy(hacc.at[k], d2d_in.at[k], ds_sem.at[k], dr_sem.at[k],
                                            device_id=dev(1), device_id_type=MESH)

    def hop1(c, axis):
        return pltpu.make_async_remote_copy(out1.at[c, axis], in1.at[c, axis], s1_sem.at[c, axis], r1_sem.at[c, axis],
                                            device_id=dev(4 if axis else 2), device_id_type=MESH)

    def hop2(c, part):
        return pltpu.make_async_remote_copy(out2.at[c, part], in2.at[c, part], s2_sem.at[c, part], r2_sem.at[c, part],
                                            device_id=dev(2 if part else 4), device_id_type=MESH)

    def combine(r):
        g = gidx(r)
        parts = []
        for e in range(nexp):
            at = e * (cap // 16) + start_s[e, g]
            parts.append(obuf[pl.ds(at, WIN // 16)].reshape(WIN, wd))
        win = jnp.concatenate(parts, axis=0)
        rows = pl.ds(pl.multiple_of(g * tok_dev, 64), tok_dev)
        lhs = jnp.concatenate([cmat[k, rows, :] for k in range(3)], axis=0)
        y = jnp.dot(lhs, win, preferred_element_type=F32)
        return y[:tok_dev] + y[tok_dev:2 * tok_dev] + y[2 * tok_dev:]

    def relay(c):
        for part in range(2):
            hop1(c, part).wait_recv()
            out2[c, part] = (kept[c, part] + in1[c, part, 1].astype(F32)).astype(BF)
            hop2(c, part).start()

    def finish(c):
        for part in range(2):
            hop2(c, part).wait_recv()
            at = pl.multiple_of(me * tok_dev + part * half, 32)
            y = tok_all[c, pl.ds(at, half), :].astype(F32) + (
                own[c, part] + in1[c, part, 0].astype(F32) + in2[c, part].astype(F32))
            outv[c, part * half:(part + 1) * half, :] = y.astype(BF)
        out_copy(c).start()

    def second(c, _):
        def pair(q, _):
            for h in range(2):
                e = q * 2 + h
                s = c * nexp + e
                slot = lax.rem(s, NO)
                wo_copy(s).wait()
                rows = pl.ds(pl.multiple_of(e * cap, 64), cap)
                y = jnp.dot(hbf[rows, :], wo[slot], preferred_element_type=F32).astype(BF)
                obuf[pl.ds(e * (cap // 16), cap // 16)] = y.reshape(cap // 16, 16, wd)

                @pl.when(s + NO < nch * nexp)
                def _():
                    wo_copy(s + NO).start()
            return 0

        lax.fori_loop(0, nexp // 2, pair, 0)
        for q, r in enumerate(RETURN_ORDER):
            hacc[c * 4 + q] = combine(r + 1)
            d2d_copy(c, q).start()
        for q, r in enumerate(RETURN_ORDER):
            y = combine(r)
            d2d_copy(c, q).wait_recv()
            y = y + d2d_in[c * 4 + q]
            if r == 6:
                out1[c, 0, 1] = y[:half].astype(BF)
                out1[c, 1, 1] = y[half:].astype(BF)
            elif r == 2:
                out1[c, 0, 0] = y[:half].astype(BF)
                kept[c, 1] = y[half:]
                hop1(c, 0).start()
            elif r == 4:
                out1[c, 1, 0] = y[half:].astype(BF)
                kept[c, 0] = y[:half]
                hop1(c, 1).start()
            else:
                own[c, 0] = y[:half]
                own[c, 1] = y[half:]

        @pl.when(c > 0)
        def _():
            relay(c - 1)

        @pl.when(c > 1)
        def _():
            finish(c - 2)
        return 0

    lax.fori_loop(0, nch, second, 0)
    relay(nch - 1)
    finish(nch - 2)
    finish(nch - 1)

    for r in range(1, 8):
        ids_copy(r).wait_send()
        gate_copy(r).wait_send()

    def drain(c, _):
        for kind in range(9):
            ag_copy(c, kind, True).wait_send()
        for q in range(4):
            d2d_copy(c, q).wait_send()
        for part in range(2):
            hop1(c, part).wait_send()
            hop2(c, part).wait_send()
        out_copy(c).wait()
        return 0

    lax.fori_loop(0, nch, drain, 0)


def solution(mesh):
    group_size = mesh.shape['row'] * mesh.shape['col']

    def device_fn(tokens, expert_ids, gate_weights, w_in, w_out):
        tok_dev, width = tokens.shape
        top_k = expert_ids.shape[1]
        nexp, _, ff = w_in.shape
        cap = tok_dev * group_size * top_k // (nexp * group_size)
        ntok = tok_dev * group_size
        nch = 8
        wd = width // nch
        half = tok_dev // 2
        dma = pltpu.SemaphoreType.DMA
        cfg = (tok_dev, cap, nexp, nch, wd, ff)
        vm = pl.BlockSpec(memory_space=pltpu.VMEM)
        hb = pl.BlockSpec(memory_space=pl.ANY)
        return pl.pallas_call(
            functools.partial(moe_kernel, cfg),
            out_shape=jax.ShapeDtypeStruct((tok_dev, width), BF),
            in_specs=[vm, vm, hb, hb, hb],
            out_specs=hb,
            scratch_shapes=[
                pltpu.VMEM((8, 8, 256), jnp.int32),
                pltpu.VMEM((8, 8, 256), F32),
                pltpu.VMEM((nch, ntok, wd), BF),
                pltpu.VMEM((nexp * cap, ntok), BF),
                pltpu.VMEM((3, ntok, nexp * WIN), BF),
                pltpu.VMEM((nexp * ff // wd, cap, wd), F32),
                pltpu.VMEM((nexp * cap, ff), BF),
                pltpu.VMEM((NI, wd, ff), BF),
                pltpu.VMEM((NO, ff, wd), BF),
                pltpu.VMEM((nexp * cap // 16, 16, wd), BF),
                pltpu.VMEM((nch * 4, tok_dev, wd), F32),
                pltpu.VMEM((nch, 2, 2, half, wd), BF),
                pltpu.VMEM((nch, 2, 2, half, wd), BF),
                pltpu.VMEM((nch, 2, half, wd), BF),
                pltpu.VMEM((nch, 2, half, wd), BF),
                pltpu.VMEM((nch, 2, half, wd), F32),
                pltpu.VMEM((nch, 2, half, wd), F32),
                pltpu.VMEM((nch, tok_dev, wd), BF),
                pltpu.VMEM((8, ntok), F32),
                pltpu.VMEM((ntok // 128, 32, 128), F32),
                pltpu.VMEM((8, 128), jnp.int32),
                pltpu.SMEM((8, 128), jnp.int32),
                dma((nch,)), dma((NI,)), dma((NO,)), dma((7,)), dma((7,)), dma((7,)), dma((7,)), dma((nch, 9)), dma((nch, 9)),
                dma((nch * 4,)), dma((nch * 4,)), dma((nch, 2)), dma((nch, 2)), dma((nch, 2)), dma((nch, 2)), dma, dma((nch,)),
            ],
            compiler_params=pltpu.CompilerParams(collective_id=0, has_side_effects=True, vmem_limit_bytes=67000000),
        )(expert_ids.T, gate_weights.T, tokens, w_in, w_out)

    token_spec = P(('data', 'row', 'col'), None)
    expert_spec = P(GRID_AXES, None, None)
    return jax.shard_map(device_fn, mesh=mesh, in_specs=(token_spec, token_spec, token_spec, expert_spec, expert_spec),
                         out_specs=token_spec, check_vma=False)
```

```python
import functools

import jax
import jax.numpy as jnp
from jax import lax
from jax.experimental import pallas as pl
from jax.experimental.pallas import tpu as pltpu
from jax.sharding import PartitionSpec as P

GRID_AXES = ('row', 'col')
MESH = pl.DeviceIdType.MESH
BF = jnp.bfloat16
F32 = jnp.float32
NI = 10
NO = 10
WIN = 64
LEAD = 2
AG_KINDS = ((0, None, 1), (0, None, 2), (0, None, 4), (2, 0, 4), (4, 1, 2), (2, None, 1), (4, None, 1), (6, 0, 1), (6, 1, 1))
RETURN_ORDER = (6, 2, 4, 0)


def moe_kernel(cfg, ids_ref, gate_ref, tok_hbm, wi_hbm, wo_hbm, out_hbm,
               ids_all, gate_all, tok_all, pmat, cmat, hacc, hbf, wi, wo, obuf, d2d_in, out1, in1, out2, in2, kept, own, outv,
               slot_buf, zbuf, start_v, start_s,
               tok_sem, wi_sem, wo_sem, ms_sem, mr_sem, gs_sem, gr_sem, as_sem, ar_sem, ds_sem, dr_sem,
               s1_sem, r1_sem, s2_sem, r2_sem, st_sem, out_sem):
    tok_dev, cap, nexp, nch, wd, ff = cfg
    ntok = 8 * tok_dev
    half = tok_dev // 2
    i = lax.axis_index('row')
    j = lax.axis_index('col')
    j_flip = j + 1 - 2 * lax.rem(j, 2)

    def rel(r):
        jj = j_flip if r & 1 else j
        if r & 2:
            jj = lax.rem(jj + 2, 4)
        ii = lax.rem(i + 1, 2) if r & 4 else i
        return ii, jj

    def dev(r):
        ii, jj = rel(r)
        return {'row': ii, 'col': jj}

    def gidx(r):
        ii, jj = rel(r)
        return ii * 4 + jj

    def rows_of(r):
        return pl.ds(pl.multiple_of(gidx(r) * tok_dev, 64), tok_dev)

    me = gidx(0)

    def tok_copy(c):
        return pltpu.make_async_copy(tok_hbm.at[:, pl.ds(c * wd, wd)], tok_all.at[c, rows_of(0), :], tok_sem.at[c])

    def wi_copy(s):
        c, e = s // nexp, lax.rem(s, nexp)
        slot = lax.rem(s, NI)
        return pltpu.make_async_copy(wi_hbm.at[e, pl.ds(pl.multiple_of(c * wd, wd), wd), :], wi.at[slot], wi_sem.at[slot])

    def wo_copy(s):
        c, e = s // nexp, lax.rem(s, nexp)
        slot = lax.rem(s, NO)
        return pltpu.make_async_copy(wo_hbm.at[e, :, pl.ds(pl.multiple_of(c * wd, wd), wd)], wo.at[slot], wo_sem.at[slot])

    def out_copy(c):
        return pltpu.make_async_copy(outv.at[c], out_hbm.at[:, pl.ds(pl.multiple_of(c * wd, wd), wd)], out_sem.at[c])

    for c in range(nch):
        tok_copy(c).start()

    def prefetch_i(s, _):
        wi_copy(s).start()
        return 0

    def prefetch_o(s, _):
        wo_copy(s).start()
        return 0

    lax.fori_loop(0, NI, prefetch_i, 0)
    lax.fori_loop(0, NO, prefetch_o, 0)
    ids_all[me] = jnp.zeros((8, 256), jnp.int32)
    ids_all[me, :, :tok_dev] = ids_ref[...]
    gate_all[me] = jnp.zeros((8, 256), F32)
    gate_all[me, :, :tok_dev] = gate_ref[...]

    bar = pltpu.get_barrier_semaphore()
    for r in range(1, 8):
        pl.semaphore_signal(bar, inc=1, device_id=dev(r), device_id_type=MESH)
    pl.semaphore_wait(bar, 7)

    def ids_copy(r):
        return pltpu.make_async_remote_copy(ids_all.at[me], ids_all.at[me], ms_sem.at[r - 1], mr_sem.at[r - 1],
                                            device_id=dev(r), device_id_type=MESH)

    def gate_copy(r):
        return pltpu.make_async_remote_copy(gate_all.at[me], gate_all.at[me], gs_sem.at[r - 1], gr_sem.at[r - 1],
                                            device_id=dev(r), device_id_type=MESH)

    def ag_copy(c, kind, mine):
        owner, part, to = AG_KINDS[kind]
        if not mine:
            owner = owner ^ to
        start, size = gidx(owner) * tok_dev, tok_dev
        if part is not None:
            start, size = start + part * half, half
        ref = tok_all.at[c, pl.ds(pl.multiple_of(start, 32), size), :]
        return pltpu.make_async_remote_copy(ref, ref, as_sem.at[c, kind], ar_sem.at[c, kind],
                                            device_id=dev(to), device_id_type=MESH)

    def send_own(c):
        tok_copy(c).wait()
        for kind in (1, 2, 0):
            ag_copy(c, kind, True).start()

    def near(c):
        ag_copy(c, 1, False).wait_recv()
        ag_copy(c, 3, True).start()
        ag_copy(c, 5, True).start()
        ag_copy(c, 2, False).wait_recv()
        ag_copy(c, 4, True).start()
        ag_copy(c, 6, True).start()

    def far(c):
        ag_copy(c, 3, False).wait_recv()
        ag_copy(c, 7, True).start()
        ag_copy(c, 4, False).wait_recv()
        ag_copy(c, 8, True).start()

    for r in range(1, 8):
        ids_copy(r).start()
        gate_copy(r).start()
    for c in range(LEAD):
        send_own(c)

    for r in range(1, 8):
        ids_copy(r).wait_recv()
        gate_copy(r).wait_recv()

    lane = lax.broadcasted_iota(jnp.int32, (8, 128), 1)

    def compact(ref):
        out = []
        for m in range(4):
            a = ref[2 * m]
            b = pltpu.roll(ref[2 * m + 1], 64, 1)
            out += [a[:, :128], jnp.where(lane < 64, a[:, 128:], b[:, :128]), b[:, 128:]]
        return out

    id_blocks, gate_blocks = compact(ids_all), compact(gate_all)
    eid = lax.broadcasted_iota(jnp.int32, (8, 128), 0) + me * nexp
    imasks, gates = [], []
    for idb, gb in zip(id_blocks, gate_blocks):
        m = jnp.zeros((8, 128), jnp.int32)
        g = jnp.zeros((8, 128), F32)
        for k in range(8):
            hit = idb[k:k + 1, :] == eid
            m = jnp.where(hit, 1, m)
            g = jnp.where(hit, gb[k:k + 1, :], g)
        imasks.append(m)
        gates.append(g)
    masks = [m.astype(F32) for m in imasks]
    nb = len(masks)
    tri = jnp.where(lax.broadcasted_iota(jnp.int32, (128, 128), 0) < lax.broadcasted_iota(jnp.int32, (128, 128), 1),
                    1.0, 0.0).astype(BF)
    cums = jnp.dot(jnp.concatenate(masks, axis=0).astype(BF), tri, preferred_element_type=F32)
    carry = jnp.zeros((8, 1), F32)
    ranks = []
    for b in range(nb):
        ranks.append(cums[b * 8:b * 8 + 8, :] + carry)
        carry = carry + jnp.sum(masks[b], axis=1, keepdims=True)
    starts, seen = [], jnp.zeros((8, 128), jnp.int32)
    table = jnp.zeros((8, 128), jnp.int32)
    for g in range(8):
        b = 3 * (g // 2) + g % 2
        before = seen + jnp.where(lane < 64, imasks[b], 0) if g % 2 else seen
        off = jnp.sum(before, axis=1, keepdims=True)
        start16 = jnp.minimum(off >> 4, (cap - WIN) // 16)
        table = jnp.where(lane == g, start16, table)
        starts.append((start16 * 16).astype(F32))
        seen = seen + imasks[b]
        if g % 2:
            seen = seen + imasks[b + 1]
    start_v[...] = table
    st = pltpu.make_async_copy(start_v, start_s, st_sem)
    st.start()
    for b in range(nb):
        m = b // 3
        if b % 3 == 0:
            start = starts[2 * m]
        elif b % 3 == 1:
            start = jnp.where(lane < 64, starts[2 * m], starts[2 * m + 1])
        else:
            start = starts[2 * m + 1]
        keep = (masks[b] > 0.0) & (ranks[b] < float(cap))
        slot_buf[:, b * 128:(b + 1) * 128] = jnp.where(keep, ranks[b], -1.0)
        g1 = gates[b].astype(BF).astype(F32)
        rem1 = gates[b] - g1
        g2 = rem1.astype(BF).astype(F32)
        g3 = rem1 - g2
        zbuf[b, 0:8, :] = jnp.where(keep, ranks[b] - start, -1.0)
        zbuf[b, 8:16, :] = g1
        zbuf[b, 16:24, :] = g2
        zbuf[b, 24:32, :] = g3

    def build_p(e, _):
        row = slot_buf[pl.ds(e, 1), :]
        pos = lax.broadcasted_iota(jnp.int32, (cap, ntok), 0).astype(F32)
        pmat[pl.ds(pl.multiple_of(e * cap, 64), cap), :] = jnp.where(pos == row, 1.0, 0.0).astype(BF)
        return 0

    nwin = nexp * WIN

    def build_c(b, _):
        z = jnp.concatenate([zbuf[b], jnp.zeros((96, 128), F32)], axis=0)
        zt = jnp.transpose(z).astype(BF)
        ex = jnp.where(lax.broadcasted_iota(jnp.int32, (128, 4 * nwin), 0)
                       == lax.broadcasted_iota(jnp.int32, (128, 4 * nwin), 1) // WIN, 1.0, 0.0).astype(BF)
        y = jnp.dot(zt, ex, preferred_element_type=F32)
        wpos = lax.rem(lax.broadcasted_iota(jnp.int32, (128, nwin), 1), WIN).astype(F32)
        hit = y[:, :nwin] == wpos
        rows = pl.ds(pl.multiple_of(b * 128, 128), 128)
        for k in range(3):
            cmat[k, rows, :] = jnp.where(hit, y[:, (k + 1) * nwin:(k + 2) * nwin], 0.0).astype(BF)
        return 0

    def zero(k, _):
        hacc[k] = jnp.zeros((cap, wd), F32)
        return 0

    def first(c, last):
        for kind in (0, 5, 6, 7, 8):
            ag_copy(c, kind, False).wait_recv()

        def pair(q, _):
            for h in range(2):
                e = q * 2 + h
                s = c * nexp + e
                slot = lax.rem(s, NI)
                rows = pl.ds(pl.multiple_of(e * cap, 64), cap)
                wi_copy(s).wait()
                bufr = jnp.dot(pmat[rows, :], tok_all[c], preferred_element_type=F32).astype(BF)
                y = jnp.dot(bufr, wi[slot], preferred_element_type=F32)
                for n in range(ff // wd):
                    yn = y[:, n * wd:(n + 1) * wd] + hacc[e * (ff // wd) + n]
                    if last:
                        hbf[rows, n * wd:(n + 1) * wd] = jax.nn.gelu(yn, approximate=True).astype(BF)
                    else:
                        hacc[e * (ff // wd) + n] = yn

                @pl.when(s + NI < nch * nexp)
                def _():
                    wi_copy(s + NI).start()
            return 0

        lax.fori_loop(0, nexp // 2, pair, 0)

    near(0)
    send_own(LEAD)
    lax.fori_loop(0, nexp, build_p, 0)
    lax.fori_loop(0, nexp * ff // wd, zero, 0)
    near(1)
    if LEAD + 1 < nch:
        send_own(LEAD + 1)
    lax.fori_loop(0, nb, build_c, 0)
    far(0)

    def step(c, _):
        @pl.when(c < nch)
        def _():
            near(c)

        @pl.when(c + LEAD < nch)
        def _():
            send_own(c + LEAD)
        first(c - 2, False)
        far(c - 1)
        return 0

    lax.fori_loop(2, nch + 1, step, 0)
    first(nch - 1, True)
    st.wait()

    def d2d_copy(c, q):
        k = c * 4 + q
        return pltpu.make_async_remote_copy(hacc.at[k], d2d_in.at[k], ds_sem.at[k], dr_sem.at[k],
                                            device_id=dev(1), device_id_type=MESH)

    def hop1(c, axis, k):
        return pltpu.make_async_remote_copy(out1.at[c, axis, k], in1.at[c, axis, k], s1_sem.at[c, axis * 2 + k],
                                            r1_sem.at[c, axis * 2 + k], device_id=dev(4 if axis else 2), device_id_type=MESH)

    def hop2(c, part):
        return pltpu.make_async_remote_copy(out2.at[c, part], in2.at[c, part], s2_sem.at[c, part], r2_sem.at[c, part],
                                            device_id=dev(2 if part else 4), device_id_type=MESH)

    def combine(r):
        g = gidx(r)
        parts = []
        for e in range(nexp):
            at = e * (cap // 16) + start_s[e, g]
            parts.append(obuf[pl.ds(at, WIN // 16)].reshape(WIN, wd))
        win = jnp.concatenate(parts, axis=0)
        rows = pl.ds(pl.multiple_of(g * tok_dev, 64), tok_dev)
        lhs = jnp.concatenate([cmat[k, rows, :] for k in range(3)], axis=0)
        y = jnp.dot(lhs, win, preferred_element_type=F32)
        return y[:tok_dev] + y[tok_dev:2 * tok_dev] + y[2 * tok_dev:]

    def relay(c):
        for part in range(2):
            hop1(c, part, 1).wait_recv()
            out2[c, part] = (kept[c, part] + in1[c, part, 1].astype(F32)).astype(BF)
            hop2(c, part).start()

    def finish(c):
        for part in range(2):
            hop1(c, part, 0).wait_recv()
            hop2(c, part).wait_recv()
            at = pl.multiple_of(me * tok_dev + part * half, 32)
            y = tok_all[c, pl.ds(at, half), :].astype(F32) + (
                own[c, part] + in1[c, part, 0].astype(F32) + in2[c, part].astype(F32))
            outv[c, part * half:(part + 1) * half, :] = y.astype(BF)
        out_copy(c).start()

    def second(c, _):
        def pair(q, _):
            for h in range(2):
                e = q * 2 + h
                s = c * nexp + e
                slot = lax.rem(s, NO)
                wo_copy(s).wait()
                rows = pl.ds(pl.multiple_of(e * cap, 64), cap)
                y = jnp.dot(hbf[rows, :], wo[slot], preferred_element_type=F32).astype(BF)
                obuf[pl.ds(e * (cap // 16), cap // 16)] = y.reshape(cap // 16, 16, wd)

                @pl.when(s + NO < nch * nexp)
                def _():
                    wo_copy(s + NO).start()
            return 0

        lax.fori_loop(0, nexp // 2, pair, 0)
        for q, r in enumerate(RETURN_ORDER):
            hacc[c * 4 + q] = combine(r + 1)
            d2d_copy(c, q).start()
        for q, r in enumerate(RETURN_ORDER):
            y = combine(r)
            d2d_copy(c, q).wait_recv()
            y = y + d2d_in[c * 4 + q]
            if r == 6:
                out1[c, 0, 1] = y[:half].astype(BF)
                out1[c, 1, 1] = y[half:].astype(BF)
                hop1(c, 0, 1).start()
                hop1(c, 1, 1).start()
            elif r == 2:
                out1[c, 0, 0] = y[:half].astype(BF)
                kept[c, 1] = y[half:]
                hop1(c, 0, 0).start()
            elif r == 4:
                out1[c, 1, 0] = y[half:].astype(BF)
                kept[c, 0] = y[:half]
                hop1(c, 1, 0).start()
            else:
                own[c, 0] = y[:half]
                own[c, 1] = y[half:]

        @pl.when(c > 0)
        def _():
            relay(c - 1)

        @pl.when(c > 1)
        def _():
            finish(c - 2)
        return 0

    lax.fori_loop(0, nch, second, 0)
    relay(nch - 1)
    finish(nch - 2)
    finish(nch - 1)

    for r in range(1, 8):
        ids_copy(r).wait_send()
        gate_copy(r).wait_send()

    def drain(c, _):
        for kind in range(9):
            ag_copy(c, kind, True).wait_send()
        for q in range(4):
            d2d_copy(c, q).wait_send()
        for part in range(2):
            hop1(c, part, 0).wait_send()
            hop1(c, part, 1).wait_send()
            hop2(c, part).wait_send()
        out_copy(c).wait()
        return 0

    lax.fori_loop(0, nch, drain, 0)


def solution(mesh):
    group_size = mesh.shape['row'] * mesh.shape['col']

    def device_fn(tokens, expert_ids, gate_weights, w_in, w_out):
        tok_dev, width = tokens.shape
        top_k = expert_ids.shape[1]
        nexp, _, ff = w_in.shape
        cap = tok_dev * group_size * top_k // (nexp * group_size)
        ntok = tok_dev * group_size
        nch = 4
        wd = width // nch
        half = tok_dev // 2
        dma = pltpu.SemaphoreType.DMA
        cfg = (tok_dev, cap, nexp, nch, wd, ff)
        vm = pl.BlockSpec(memory_space=pltpu.VMEM)
        hb = pl.BlockSpec(memory_space=pl.ANY)
        return pl.pallas_call(
            functools.partial(moe_kernel, cfg),
            out_shape=jax.ShapeDtypeStruct((tok_dev, width), BF),
            in_specs=[vm, vm, hb, hb, hb],
            out_specs=hb,
            scratch_shapes=[
                pltpu.VMEM((8, 8, 256), jnp.int32),
                pltpu.VMEM((8, 8, 256), F32),
                pltpu.VMEM((nch, ntok, wd), BF),
                pltpu.VMEM((nexp * cap, ntok), BF),
                pltpu.VMEM((3, ntok, nexp * WIN), BF),
                pltpu.VMEM((nexp * ff // wd, cap, wd), F32),
                pltpu.VMEM((nexp * cap, ff), BF),
                pltpu.VMEM((NI, wd, ff), BF),
                pltpu.VMEM((NO, ff, wd), BF),
                pltpu.VMEM((nexp * cap // 16, 16, wd), BF),
                pltpu.VMEM((nch * 4, tok_dev, wd), F32),
                pltpu.VMEM((nch, 2, 2, half, wd), BF),
                pltpu.VMEM((nch, 2, 2, half, wd), BF),
                pltpu.VMEM((nch, 2, half, wd), BF),
                pltpu.VMEM((nch, 2, half, wd), BF),
                pltpu.VMEM((nch, 2, half, wd), F32),
                pltpu.VMEM((nch, 2, half, wd), F32),
                pltpu.VMEM((nch, tok_dev, wd), BF),
                pltpu.VMEM((8, ntok), F32),
                pltpu.VMEM((ntok // 128, 32, 128), F32),
                pltpu.VMEM((8, 128), jnp.int32),
                pltpu.SMEM((8, 128), jnp.int32),
                dma((nch,)), dma((NI,)), dma((NO,)), dma((7,)), dma((7,)), dma((7,)), dma((7,)), dma((nch, 9)), dma((nch, 9)),
                dma((nch * 4,)), dma((nch * 4,)), dma((nch, 4)), dma((nch, 4)), dma((nch, 2)), dma((nch, 2)), dma, dma((nch,)),
            ],
            compiler_params=pltpu.CompilerParams(collective_id=0, has_side_effects=True, vmem_limit_bytes=67000000),
        )(expert_ids.T, gate_weights.T, tokens, w_in, w_out)

    token_spec = P(('data', 'row', 'col'), None)
    expert_spec = P(GRID_AXES, None, None)
    return jax.shard_map(device_fn, mesh=mesh, in_specs=(token_spec, token_spec, token_spec, expert_spec, expert_spec),
                         out_specs=token_spec, check_vma=False)
```

```python
import functools

import jax
import jax.numpy as jnp
from jax import lax
from jax.experimental import pallas as pl
from jax.experimental.pallas import tpu as pltpu
from jax.sharding import PartitionSpec as P

GRID_AXES = ('row', 'col')
MESH = pl.DeviceIdType.MESH
BF = jnp.bfloat16
F32 = jnp.float32
NI = 10
NO = 10
WIN = 64
LEAD = 2
AG_KINDS = ((0, None, 1), (0, None, 2), (0, None, 4), (2, 0, 4), (4, 1, 2), (2, None, 1), (4, None, 1), (6, 0, 1), (6, 1, 1))
RETURN_ORDER = (6, 2, 4, 0)


def moe_kernel(cfg, ids_ref, gate_ref, tok_hbm, wi_hbm, wo_hbm, out_hbm,
               ids_all, gate_all, tok_all, pmat, cmat, hacc, hbf, wi, wo, obuf, d2d_in, out1, in1, out2, in2, kept, own, mine, outv,
               slot_buf, zbuf, start_v, start_s,
               tok_sem, wi_sem, wo_sem, ms_sem, mr_sem, gs_sem, gr_sem, as_sem, ar_sem, ds_sem, dr_sem,
               s1_sem, r1_sem, s2_sem, r2_sem, st_sem, out_sem):
    tok_dev, cap, nexp, nch, wd, ff = cfg
    ntok = 8 * tok_dev
    half = tok_dev // 2
    i = lax.axis_index('row')
    j = lax.axis_index('col')
    j_flip = j + 1 - 2 * lax.rem(j, 2)

    def rel(r):
        jj = j_flip if r & 1 else j
        if r & 2:
            jj = lax.rem(jj + 2, 4)
        ii = lax.rem(i + 1, 2) if r & 4 else i
        return ii, jj

    def dev(r):
        ii, jj = rel(r)
        return {'row': ii, 'col': jj}

    def gidx(r):
        ii, jj = rel(r)
        return ii * 4 + jj

    def rows_of(r):
        return pl.ds(pl.multiple_of(gidx(r) * tok_dev, 64), tok_dev)

    me = gidx(0)

    def tok_copy(c):
        return pltpu.make_async_copy(tok_hbm.at[:, pl.ds(c * wd, wd)], tok_all.at[c, rows_of(0), :], tok_sem.at[c])

    def wi_copy(s):
        c, e = s // nexp, lax.rem(s, nexp)
        slot = lax.rem(s, NI)
        return pltpu.make_async_copy(wi_hbm.at[e, pl.ds(pl.multiple_of(c * wd, wd), wd), :], wi.at[slot], wi_sem.at[slot])

    def wo_copy(s):
        c, e = s // nexp, lax.rem(s, nexp)
        slot = lax.rem(s, NO)
        return pltpu.make_async_copy(wo_hbm.at[e, :, pl.ds(pl.multiple_of(c * wd, wd), wd)], wo.at[slot], wo_sem.at[slot])

    def out_copy(c):
        return pltpu.make_async_copy(outv.at[c], out_hbm.at[:, pl.ds(pl.multiple_of(c * wd, wd), wd)], out_sem.at[c])

    for c in range(nch):
        tok_copy(c).start()

    def prefetch_i(s, _):
        wi_copy(s).start()
        return 0

    def prefetch_o(s, _):
        wo_copy(s).start()
        return 0

    lax.fori_loop(0, NI, prefetch_i, 0)
    lax.fori_loop(0, NO, prefetch_o, 0)
    ids_all[me] = jnp.zeros((8, 256), jnp.int32)
    ids_all[me, :, :tok_dev] = ids_ref[...]
    gate_all[me] = jnp.zeros((8, 256), F32)
    gate_all[me, :, :tok_dev] = gate_ref[...]

    bar = pltpu.get_barrier_semaphore()
    for r in range(1, 8):
        pl.semaphore_signal(bar, inc=1, device_id=dev(r), device_id_type=MESH)
    pl.semaphore_wait(bar, 7)

    def ids_copy(r):
        return pltpu.make_async_remote_copy(ids_all.at[me], ids_all.at[me], ms_sem.at[r - 1], mr_sem.at[r - 1],
                                            device_id=dev(r), device_id_type=MESH)

    def gate_copy(r):
        return pltpu.make_async_remote_copy(gate_all.at[me], gate_all.at[me], gs_sem.at[r - 1], gr_sem.at[r - 1],
                                            device_id=dev(r), device_id_type=MESH)

    def ag_copy(c, kind, mine):
        owner, part, to = AG_KINDS[kind]
        if not mine:
            owner = owner ^ to
        start, size = gidx(owner) * tok_dev, tok_dev
        if part is not None:
            start, size = start + part * half, half
        ref = tok_all.at[c, pl.ds(pl.multiple_of(start, 32), size), :]
        return pltpu.make_async_remote_copy(ref, ref, as_sem.at[c, kind], ar_sem.at[c, kind],
                                            device_id=dev(to), device_id_type=MESH)

    def send_own(c):
        tok_copy(c).wait()
        for kind in (1, 2, 0):
            ag_copy(c, kind, True).start()

    def near(c):
        ag_copy(c, 1, False).wait_recv()
        ag_copy(c, 3, True).start()
        ag_copy(c, 5, True).start()
        ag_copy(c, 2, False).wait_recv()
        ag_copy(c, 4, True).start()
        ag_copy(c, 6, True).start()

    def far(c):
        ag_copy(c, 3, False).wait_recv()
        ag_copy(c, 7, True).start()
        ag_copy(c, 4, False).wait_recv()
        ag_copy(c, 8, True).start()

    for r in range(1, 8):
        ids_copy(r).start()
        gate_copy(r).start()
    for c in range(LEAD):
        send_own(c)

    for r in range(1, 8):
        ids_copy(r).wait_recv()
        gate_copy(r).wait_recv()

    lane = lax.broadcasted_iota(jnp.int32, (8, 128), 1)

    def compact(ref):
        out = []
        for m in range(4):
            a = ref[2 * m]
            b = pltpu.roll(ref[2 * m + 1], 64, 1)
            out += [a[:, :128], jnp.where(lane < 64, a[:, 128:], b[:, :128]), b[:, 128:]]
        return out

    id_blocks, gate_blocks = compact(ids_all), compact(gate_all)
    eid = lax.broadcasted_iota(jnp.int32, (8, 128), 0) + me * nexp
    imasks, gates = [], []
    for idb, gb in zip(id_blocks, gate_blocks):
        m = jnp.zeros((8, 128), jnp.int32)
        g = jnp.zeros((8, 128), F32)
        for k in range(8):
            hit = idb[k:k + 1, :] == eid
            m = jnp.where(hit, 1, m)
            g = jnp.where(hit, gb[k:k + 1, :], g)
        imasks.append(m)
        gates.append(g)
    masks = [m.astype(F32) for m in imasks]
    nb = len(masks)
    tri = jnp.where(lax.broadcasted_iota(jnp.int32, (128, 128), 0) < lax.broadcasted_iota(jnp.int32, (128, 128), 1),
                    1.0, 0.0).astype(BF)
    cums = jnp.dot(jnp.concatenate(masks, axis=0).astype(BF), tri, preferred_element_type=F32)
    carry = jnp.zeros((8, 1), F32)
    ranks = []
    for b in range(nb):
        ranks.append(cums[b * 8:b * 8 + 8, :] + carry)
        carry = carry + jnp.sum(masks[b], axis=1, keepdims=True)
    starts, seen = [], jnp.zeros((8, 128), jnp.int32)
    table = jnp.zeros((8, 128), jnp.int32)
    for g in range(8):
        b = 3 * (g // 2) + g % 2
        before = seen + jnp.where(lane < 64, imasks[b], 0) if g % 2 else seen
        off = jnp.sum(before, axis=1, keepdims=True)
        start16 = jnp.minimum(off >> 4, (cap - WIN) // 16)
        table = jnp.where(lane == g, start16, table)
        starts.append((start16 * 16).astype(F32))
        seen = seen + imasks[b]
        if g % 2:
            seen = seen + imasks[b + 1]
    start_v[...] = table
    st = pltpu.make_async_copy(start_v, start_s, st_sem)
    st.start()
    for b in range(nb):
        m = b // 3
        if b % 3 == 0:
            start = starts[2 * m]
        elif b % 3 == 1:
            start = jnp.where(lane < 64, starts[2 * m], starts[2 * m + 1])
        else:
            start = starts[2 * m + 1]
        keep = (masks[b] > 0.0) & (ranks[b] < float(cap))
        slot_buf[:, b * 128:(b + 1) * 128] = jnp.where(keep, ranks[b], -1.0)
        g1 = gates[b].astype(BF).astype(F32)
        rem1 = gates[b] - g1
        g2 = rem1.astype(BF).astype(F32)
        g3 = rem1 - g2
        zbuf[b, 0:8, :] = jnp.where(keep, ranks[b] - start, -1.0)
        zbuf[b, 8:16, :] = g1
        zbuf[b, 16:24, :] = g2
        zbuf[b, 24:32, :] = g3

    def build_p(e, _):
        row = slot_buf[pl.ds(e, 1), :]
        pos = lax.broadcasted_iota(jnp.int32, (cap, ntok), 0).astype(F32)
        pmat[pl.ds(pl.multiple_of(e * cap, 64), cap), :] = jnp.where(pos == row, 1.0, 0.0).astype(BF)
        return 0

    nwin = nexp * WIN

    def build_c(b, _):
        z = jnp.concatenate([zbuf[b], jnp.zeros((96, 128), F32)], axis=0)
        zt = jnp.transpose(z).astype(BF)
        ex = jnp.where(lax.broadcasted_iota(jnp.int32, (128, 4 * nwin), 0)
                       == lax.broadcasted_iota(jnp.int32, (128, 4 * nwin), 1) // WIN, 1.0, 0.0).astype(BF)
        y = jnp.dot(zt, ex, preferred_element_type=F32)
        wpos = lax.rem(lax.broadcasted_iota(jnp.int32, (128, nwin), 1), WIN).astype(F32)
        hit = y[:, :nwin] == wpos
        rows = pl.ds(pl.multiple_of(b * 128, 128), 128)
        for k in range(3):
            cmat[k, rows, :] = jnp.where(hit, y[:, (k + 1) * nwin:(k + 2) * nwin], 0.0).astype(BF)
        return 0

    def arrived(c):
        for kind in (0, 5, 6, 7, 8):
            ag_copy(c, kind, False).wait_recv()

    def first(c, part):
        experts = range(part * (nexp // 2), (part + 1) * (nexp // 2))
        for e in experts:
            wi_copy(c * nexp + e).wait()

        def dispatch(e):
            return jnp.dot(pmat[e * cap:(e + 1) * cap, :], tok_all[c], preferred_element_type=F32).astype(BF)

        def expand(e, rows):
            y = jnp.dot(rows, wi[(c * nexp + e) % NI], preferred_element_type=F32)
            for n in range(ff // wd):
                yn = y[:, n * wd:(n + 1) * wd]
                if c:
                    yn = yn + hacc[e * (ff // wd) + n]
                if c == nch - 1:
                    hbf[e * cap:(e + 1) * cap, n * wd:(n + 1) * wd] = jax.nn.gelu(yn, approximate=True).astype(BF)
                else:
                    hacc[e * (ff // wd) + n] = yn

        ready = None
        for e in experts:
            rows = dispatch(e)
            if ready is not None:
                expand(*ready)
            ready = (e, rows)
        expand(*ready)
        for e in experts:
            s = c * nexp + e
            if s + NI < nch * nexp:
                wi_copy(s + NI).start()

    lax.fori_loop(0, nexp, build_p, 0)
    lax.fori_loop(0, nb, build_c, 0)
    near(0)
    send_own(2)
    near(1)
    send_own(3)
    far(0)
    arrived(0)
    first(0, 0)
    first(0, 1)
    near(2)
    far(1)
    arrived(1)
    first(1, 0)
    near(3)
    first(1, 1)
    far(2)
    arrived(2)
    first(2, 0)
    far(3)
    first(2, 1)
    arrived(3)
    first(3, 0)
    first(3, 1)
    st.wait()

    def d2d_copy(c, q):
        k = c * 4 + q
        return pltpu.make_async_remote_copy(hacc.at[k], d2d_in.at[k], ds_sem.at[k], dr_sem.at[k],
                                            device_id=dev(1), device_id_type=MESH)

    def hop1(c, axis, k):
        return pltpu.make_async_remote_copy(out1.at[c, axis, k], in1.at[c, axis, k], s1_sem.at[c, axis * 2 + k],
                                            r1_sem.at[c, axis * 2 + k], device_id=dev(4 if axis else 2), device_id_type=MESH)

    def hop2(c, part):
        return pltpu.make_async_remote_copy(out2.at[c, part], in2.at[c, part], s2_sem.at[c, part], r2_sem.at[c, part],
                                            device_id=dev(2 if part else 4), device_id_type=MESH)

    def combine(r):
        g = gidx(r)
        parts = []
        for e in range(nexp):
            at = e * (cap // 16) + start_s[e, g]
            parts.append(obuf[pl.ds(at, WIN // 16)].reshape(WIN, wd))
        win = jnp.concatenate(parts, axis=0)
        rows = pl.ds(pl.multiple_of(g * tok_dev, 64), tok_dev)
        lhs = jnp.concatenate([cmat[k, rows, :] for k in range(3)], axis=0)
        y = jnp.dot(lhs, win, preferred_element_type=F32)
        return y[:tok_dev] + y[tok_dev:2 * tok_dev] + y[2 * tok_dev:]

    def relay(c):
        for part in range(2):
            hop1(c, part, 1).wait_recv()
            out2[c, part] = (kept[c, part] + in1[c, part, 1].astype(F32)).astype(BF)
            hop2(c, part).start()

    def finish(c):
        for part in range(2):
            hop1(c, part, 0).wait_recv()
            hop2(c, part).wait_recv()
            at = pl.multiple_of(me * tok_dev + part * half, 32)
            y = tok_all[c, pl.ds(at, half), :].astype(F32) + (
                own[c, part] + in1[c, part, 0].astype(F32) + in2[c, part].astype(F32))
            outv[c, part * half:(part + 1) * half, :] = y.astype(BF)
        out_copy(c).start()

    def second(c, _):
        for part in range(2):
            experts = range(part * (nexp // 2), (part + 1) * (nexp // 2))
            for e in experts:
                wo_copy(c * nexp + e).wait()
            for e in experts:
                slot = lax.rem(c * nexp + e, NO)
                y = jnp.dot(hbf[e * cap:(e + 1) * cap, :], wo[slot], preferred_element_type=F32).astype(BF)
                obuf[e * (cap // 16):(e + 1) * (cap // 16)] = y.reshape(cap // 16, 16, wd)
            for e in experts:
                s = c * nexp + e

                @pl.when(s + NO < nch * nexp)
                def _():
                    wo_copy(s + NO).start()

        for q, r in enumerate(RETURN_ORDER):
            hacc[c * 4 + q] = combine(r + 1)
        for q in range(4):
            d2d_copy(c, q).start()
        for q, r in enumerate(RETURN_ORDER):
            mine[q] = combine(r)
        for q, r in enumerate(RETURN_ORDER):
            d2d_copy(c, q).wait_recv()
            y = mine[q] + d2d_in[c * 4 + q]
            if r == 6:
                out1[c, 0, 1] = y[:half].astype(BF)
                out1[c, 1, 1] = y[half:].astype(BF)
                hop1(c, 0, 1).start()
                hop1(c, 1, 1).start()
            elif r == 2:
                out1[c, 0, 0] = y[:half].astype(BF)
                kept[c, 1] = y[half:]
                hop1(c, 0, 0).start()
            elif r == 4:
                out1[c, 1, 0] = y[half:].astype(BF)
                kept[c, 0] = y[:half]
                hop1(c, 1, 0).start()
            else:
                own[c, 0] = y[:half]
                own[c, 1] = y[half:]

        @pl.when(c > 0)
        def _():
            relay(c - 1)

        @pl.when(c > 1)
        def _():
            finish(c - 2)
        return 0

    lax.fori_loop(0, nch, second, 0)
    relay(nch - 1)
    finish(nch - 2)
    finish(nch - 1)

    for r in range(1, 8):
        ids_copy(r).wait_send()
        gate_copy(r).wait_send()

    def drain(c, _):
        for kind in range(9):
            ag_copy(c, kind, True).wait_send()
        for q in range(4):
            d2d_copy(c, q).wait_send()
        for part in range(2):
            hop1(c, part, 0).wait_send()
            hop1(c, part, 1).wait_send()
            hop2(c, part).wait_send()
        out_copy(c).wait()
        return 0

    lax.fori_loop(0, nch, drain, 0)


def solution(mesh):
    group_size = mesh.shape['row'] * mesh.shape['col']

    def device_fn(tokens, expert_ids, gate_weights, w_in, w_out):
        tok_dev, width = tokens.shape
        top_k = expert_ids.shape[1]
        nexp, _, ff = w_in.shape
        cap = tok_dev * group_size * top_k // (nexp * group_size)
        ntok = tok_dev * group_size
        nch = 4
        wd = width // nch
        half = tok_dev // 2
        dma = pltpu.SemaphoreType.DMA
        cfg = (tok_dev, cap, nexp, nch, wd, ff)
        vm = pl.BlockSpec(memory_space=pltpu.VMEM)
        hb = pl.BlockSpec(memory_space=pl.ANY)
        return pl.pallas_call(
            functools.partial(moe_kernel, cfg),
            out_shape=jax.ShapeDtypeStruct((tok_dev, width), BF),
            in_specs=[vm, vm, hb, hb, hb],
            out_specs=hb,
            scratch_shapes=[
                pltpu.VMEM((8, 8, 256), jnp.int32),
                pltpu.VMEM((8, 8, 256), F32),
                pltpu.VMEM((nch, ntok, wd), BF),
                pltpu.VMEM((nexp * cap, ntok), BF),
                pltpu.VMEM((3, ntok, nexp * WIN), BF),
                pltpu.VMEM((nexp * ff // wd, cap, wd), F32),
                pltpu.VMEM((nexp * cap, ff), BF),
                pltpu.VMEM((NI, wd, ff), BF),
                pltpu.VMEM((NO, ff, wd), BF),
                pltpu.VMEM((nexp * cap // 16, 16, wd), BF),
                pltpu.VMEM((nch * 4, tok_dev, wd), F32),
                pltpu.VMEM((nch, 2, 2, half, wd), BF),
                pltpu.VMEM((nch, 2, 2, half, wd), BF),
                pltpu.VMEM((nch, 2, half, wd), BF),
                pltpu.VMEM((nch, 2, half, wd), BF),
                pltpu.VMEM((nch, 2, half, wd), F32),
                pltpu.VMEM((nch, 2, half, wd), F32),
                pltpu.VMEM((4, tok_dev, wd), F32),
                pltpu.VMEM((nch, tok_dev, wd), BF),
                pltpu.VMEM((8, ntok), F32),
                pltpu.VMEM((ntok // 128, 32, 128), F32),
                pltpu.VMEM((8, 128), jnp.int32),
                pltpu.SMEM((8, 128), jnp.int32),
                dma((nch,)), dma((NI,)), dma((NO,)), dma((7,)), dma((7,)), dma((7,)), dma((7,)), dma((nch, 9)), dma((nch, 9)),
                dma((nch * 4,)), dma((nch * 4,)), dma((nch, 4)), dma((nch, 4)), dma((nch, 2)), dma((nch, 2)), dma, dma((nch,)),
            ],
            compiler_params=pltpu.CompilerParams(collective_id=0, has_side_effects=True, vmem_limit_bytes=67000000),
        )(expert_ids.T, gate_weights.T, tokens, w_in, w_out)

    token_spec = P(('data', 'row', 'col'), None)
    expert_spec = P(GRID_AXES, None, None)
    return jax.shard_map(device_fn, mesh=mesh, in_specs=(token_spec, token_spec, token_spec, expert_spec, expert_spec),
                         out_specs=token_spec, check_vma=False)
```

```python
import functools

import jax
import jax.numpy as jnp
from jax import lax
from jax.experimental import pallas as pl
from jax.experimental.pallas import tpu as pltpu
from jax.sharding import PartitionSpec as P

NS = jax.named_scope
GRID_AXES = ('row', 'col')
MESH = pl.DeviceIdType.MESH
BF = jnp.bfloat16
F32 = jnp.float32
WIN = 64
LEAD = 2
AG_KINDS = ((0, None, 1), (0, None, 2), (0, None, 4), (2, 0, 4), (4, 1, 2), (2, None, 1), (4, None, 1), (6, 0, 1), (6, 1, 1))
RETURN_ORDER = (6, 2, 4, 0)


def moe_kernel(cfg, ids_hbm, gate_hbm, tok_hbm, wi_hbm, wo_hbm, out_hbm,
               ids_all, gate_all, tok_all, pmat, cmat, hacc, hbf, wi, wo, obuf, d2d_in, out1, in1, out2, in2, kept, own, mine, outv,
               ids_v, gate_v, slot_buf, zbuf, start_v, start_s,
               tok_sem, wi_sem, wo_sem, ms_sem, mr_sem, gs_sem, gr_sem, as_sem, ar_sem, ds_sem, dr_sem,
               s1_sem, r1_sem, s2_sem, rf_sem, st_sem, out_sem, id_sem, gate_sem):
    tok_dev, cap, nexp, nch, wd, ff = cfg
    ntok = 8 * tok_dev
    half = tok_dev // 2
    i = lax.axis_index('row')
    j = lax.axis_index('col')
    j_flip = j + 1 - 2 * lax.rem(j, 2)

    def rel(r):
        jj = j_flip if r & 1 else j
        if r & 2:
            jj = lax.rem(jj + 2, 4)
        ii = lax.rem(i + 1, 2) if r & 4 else i
        return ii, jj

    def dev(r):
        ii, jj = rel(r)
        return {'row': ii, 'col': jj}

    def gidx(r):
        ii, jj = rel(r)
        return ii * 4 + jj

    def rows_of(r):
        return pl.ds(pl.multiple_of(gidx(r) * tok_dev, 64), tok_dev)

    me = gidx(0)

    def tok_copy(c):
        return pltpu.make_async_copy(tok_hbm.at[:, pl.ds(c * wd, wd)], tok_all.at[c, rows_of(0), :], tok_sem.at[c])

    nh = nexp // 2

    def wi_copy(c, p):
        return pltpu.make_async_copy(wi_hbm.at[p * nh:(p + 1) * nh, pl.ds(c * wd, wd), :], wi.at[p], wi_sem.at[p])

    def wo_copy(c, p):
        return pltpu.make_async_copy(wo_hbm.at[p * nh:(p + 1) * nh, :, pl.ds(pl.multiple_of(c * wd, wd), wd)], wo.at[p],
                                     wo_sem.at[p])

    def out_copy(c):
        return pltpu.make_async_copy(outv.at[c], out_hbm.at[:, pl.ds(pl.multiple_of(c * wd, wd), wd)], out_sem.at[c])

    bar = pltpu.get_barrier_semaphore()
    for r in range(1, 8):
        pl.semaphore_signal(bar, inc=1, device_id=dev(r), device_id_type=MESH)
    ids_in = pltpu.make_async_copy(ids_hbm, ids_v, id_sem)
    gate_in = pltpu.make_async_copy(gate_hbm, gate_v, gate_sem)
    ids_in.start()
    gate_in.start()
    for c in range(nch):
        tok_copy(c).start()
    for p in range(2):
        wi_copy(0, p).start()
    for p in range(2):
        wo_copy(0, p).start()
    ids_all[me] = jnp.zeros((8, 256), jnp.int32)
    gate_all[me] = jnp.zeros((8, 256), F32)
    ids_in.wait()
    gate_in.wait()
    ids_all[me, :, :tok_dev] = ids_v[...]
    gate_all[me, :, :tok_dev] = gate_v[...]
    with NS('barrier'):
        pl.semaphore_wait(bar, 7)

    def ids_copy(r):
        return pltpu.make_async_remote_copy(ids_all.at[me], ids_all.at[me], ms_sem, mr_sem,
                                            device_id=dev(r), device_id_type=MESH)

    def gate_copy(r):
        return pltpu.make_async_remote_copy(gate_all.at[me], gate_all.at[me], gs_sem, gr_sem,
                                            device_id=dev(r), device_id_type=MESH)

    def ag_copy(c, kind, mine):
        owner, part, to = AG_KINDS[kind]
        if not mine:
            owner = owner ^ to
        start, size = gidx(owner) * tok_dev, tok_dev
        if part is not None:
            start, size = start + part * half, half
        ref = tok_all.at[c, pl.ds(pl.multiple_of(start, 32), size), :]
        return pltpu.make_async_remote_copy(ref, ref, as_sem, ar_sem.at[c, kind if kind in (1, 2, 3, 4) else 0],
                                            device_id=dev(to), device_id_type=MESH)

    def send_own(c):
        tok_copy(c).wait()
        for kind in (1, 2, 0):
            ag_copy(c, kind, True).start()

    def near(c):
        with NS('near_x'):
            ag_copy(c, 1, False).wait_recv()
        ag_copy(c, 3, True).start()
        ag_copy(c, 5, True).start()
        with NS('near_y'):
            ag_copy(c, 2, False).wait_recv()
        ag_copy(c, 4, True).start()
        ag_copy(c, 6, True).start()

    def far(c):
        with NS('far_a'):
            ag_copy(c, 3, False).wait_recv()
        ag_copy(c, 7, True).start()
        with NS('far_b'):
            ag_copy(c, 4, False).wait_recv()
        ag_copy(c, 8, True).start()

    for r in range(1, 8):
        ids_copy(r).start()
        gate_copy(r).start()
    for c in range(LEAD):
        send_own(c)

    def all_of(ref, send, recv):
        return pltpu.make_async_remote_copy(ref, ref, send, recv, device_id=dev(1), device_id_type=MESH)

    all_ids = all_of(ids_all.at[0:7], ms_sem, mr_sem)
    all_gates = all_of(gate_all.at[0:7], gs_sem, gr_sem)
    with NS('meta_wait'):
        all_ids.wait_recv()
        all_gates.wait_recv()

    lane = lax.broadcasted_iota(jnp.int32, (8, 128), 1)

    def compact(ref):
        out = []
        for m in range(4):
            a = ref[2 * m]
            b = pltpu.roll(ref[2 * m + 1], 64, 1)
            out += [a[:, :128], jnp.where(lane < 64, a[:, 128:], b[:, :128]), b[:, 128:]]
        return out

    id_blocks, gate_blocks = compact(ids_all), compact(gate_all)
    eid = lax.broadcasted_iota(jnp.int32, (8, 128), 0) + me * nexp
    imasks, gates = [], []
    for idb, gb in zip(id_blocks, gate_blocks):
        m = jnp.zeros((8, 128), jnp.int32)
        g = jnp.zeros((8, 128), F32)
        for k in range(8):
            hit = idb[k:k + 1, :] == eid
            m = jnp.where(hit, 1, m)
            g = jnp.where(hit, gb[k:k + 1, :], g)
        imasks.append(m)
        gates.append(g)
    masks = [m.astype(F32) for m in imasks]
    nb = len(masks)
    tri = jnp.where(lax.broadcasted_iota(jnp.int32, (128, 128), 0) < lax.broadcasted_iota(jnp.int32, (128, 128), 1),
                    1.0, 0.0).astype(BF)
    cums = jnp.dot(jnp.concatenate(masks, axis=0).astype(BF), tri, preferred_element_type=F32)
    carry = jnp.zeros((8, 1), F32)
    ranks = []
    for b in range(nb):
        ranks.append(cums[b * 8:b * 8 + 8, :] + carry)
        carry = carry + jnp.sum(masks[b], axis=1, keepdims=True)
    starts, seen = [], jnp.zeros((8, 128), jnp.int32)
    table = jnp.zeros((8, 128), jnp.int32)
    for g in range(8):
        b = 3 * (g // 2) + g % 2
        before = seen + jnp.where(lane < 64, imasks[b], 0) if g % 2 else seen
        off = jnp.sum(before, axis=1, keepdims=True)
        start16 = jnp.minimum(off >> 4, (cap - WIN) // 16)
        table = jnp.where(lane == g, start16, table)
        starts.append((start16 * 16).astype(F32))
        seen = seen + imasks[b]
        if g % 2:
            seen = seen + imasks[b + 1]
    start_v[...] = table
    st = pltpu.make_async_copy(start_v, start_s, st_sem)
    st.start()
    for b in range(nb):
        m = b // 3
        if b % 3 == 0:
            start = starts[2 * m]
        elif b % 3 == 1:
            start = jnp.where(lane < 64, starts[2 * m], starts[2 * m + 1])
        else:
            start = starts[2 * m + 1]
        keep = (masks[b] > 0.0) & (ranks[b] < float(cap))
        slot_buf[:, b * 128:(b + 1) * 128] = jnp.where(keep, ranks[b], -1.0)
        g1 = gates[b].astype(BF).astype(F32)
        rem1 = gates[b] - g1
        g2 = rem1.astype(BF).astype(F32)
        g3 = rem1 - g2
        zbuf[b, 0:8, :] = jnp.where(keep, ranks[b] - start, -1.0)
        zbuf[b, 8:16, :] = g1
        zbuf[b, 16:24, :] = g2
        zbuf[b, 24:32, :] = g3

    def build_p(e, _):
        row = slot_buf[pl.ds(e, 1), :]
        pos = lax.broadcasted_iota(jnp.int32, (cap, ntok), 0).astype(F32)
        pmat[pl.ds(pl.multiple_of(e * cap, 64), cap), :] = jnp.where(pos == row, 1.0, 0.0).astype(BF)
        return 0

    nwin = nexp * WIN

    def build_c(b, _):
        z = jnp.concatenate([zbuf[b], jnp.zeros((96, 128), F32)], axis=0)
        zt = jnp.transpose(z).astype(BF)
        ex = jnp.where(lax.broadcasted_iota(jnp.int32, (128, 4 * nwin), 0)
                       == lax.broadcasted_iota(jnp.int32, (128, 4 * nwin), 1) // WIN, 1.0, 0.0).astype(BF)
        y = jnp.dot(zt, ex, preferred_element_type=F32)
        wpos = lax.rem(lax.broadcasted_iota(jnp.int32, (128, nwin), 1), WIN).astype(F32)
        hit = y[:, :nwin] == wpos
        rows = pl.ds(pl.multiple_of(b * 128, 128), 128)
        for k in range(3):
            cmat[k, rows, :] = jnp.where(hit, y[:, (k + 1) * nwin:(k + 2) * nwin], 0.0).astype(BF)
        return 0

    def arrived(c):
        with NS('arrived'):
            all_of(tok_all.at[c, 0:4 * tok_dev, :], as_sem, ar_sem.at[c, 0]).wait_recv()

    def first(c, part):
        experts = range(part * (nexp // 2), (part + 1) * (nexp // 2))
        with NS('first'):
            wi_copy(c, part).wait()

        def dispatch(e):
            return jnp.dot(pmat[e * cap:(e + 1) * cap, :], tok_all[c], preferred_element_type=F32).astype(BF)

        def expand(e, rows):
            y = jnp.dot(rows, wi[part, e % nh], preferred_element_type=F32)
            for n in range(ff // wd):
                yn = y[:, n * wd:(n + 1) * wd]
                if c:
                    yn = yn + hacc[e * (ff // wd) + n]
                if c == nch - 1:
                    hbf[e * cap:(e + 1) * cap, n * wd:(n + 1) * wd] = jax.nn.gelu(yn, approximate=True).astype(BF)
                else:
                    hacc[e * (ff // wd) + n] = yn

        ready = None
        for e in experts:
            rows = dispatch(e)
            if ready is not None:
                expand(*ready)
            ready = (e, rows)
        expand(*ready)
        if c + 1 < nch:
            wi_copy(c + 1, part).start()

    lax.fori_loop(0, nexp, build_p, 0)
    lax.fori_loop(0, nb, build_c, 0)
    near(0)
    send_own(2)
    near(1)
    send_own(3)
    far(0)
    arrived(0)
    first(0, 0)
    first(0, 1)
    near(2)
    far(1)
    arrived(1)
    first(1, 0)
    near(3)
    first(1, 1)
    far(2)
    arrived(2)
    first(2, 0)
    far(3)
    first(2, 1)
    arrived(3)
    first(3, 0)
    first(3, 1)
    st.wait()

    def d2d_copy(c, q):
        k = c * 4 + q
        return pltpu.make_async_remote_copy(hacc.at[k], d2d_in.at[k], ds_sem, dr_sem.at[k],
                                            device_id=dev(1), device_id_type=MESH)

    def hop1(c, axis, k):
        recv = r1_sem.at[c, axis] if k else rf_sem.at[c]
        return pltpu.make_async_remote_copy(out1.at[c, axis, k], in1.at[c, axis, k], s1_sem, recv,
                                            device_id=dev(4 if axis else 2), device_id_type=MESH)

    def hop2(c, part):
        return pltpu.make_async_remote_copy(out2.at[c, part], in2.at[c, part], s2_sem, rf_sem.at[c],
                                            device_id=dev(2 if part else 4), device_id_type=MESH)

    def combine(r):
        g = gidx(r)
        parts = []
        for e in range(nexp):
            at = e * (cap // 16) + start_s[e, g]
            parts.append(obuf[pl.ds(at, WIN // 16)].reshape(WIN, wd))
        win = jnp.concatenate(parts, axis=0)
        rows = pl.ds(pl.multiple_of(g * tok_dev, 64), tok_dev)
        lhs = jnp.concatenate([cmat[k, rows, :] for k in range(3)], axis=0)
        y = jnp.dot(lhs, win, preferred_element_type=F32)
        return y[:tok_dev] + y[tok_dev:2 * tok_dev] + y[2 * tok_dev:]

    def relay(c):
        for part in range(2):
            with NS('relay'):
                hop1(c, part, 1).wait_recv()
            out2[c, part] = (kept[c, part] + in1[c, part, 1].astype(F32)).astype(BF)
            hop2(c, part).start()

    def finish(c):
        with NS('finish'):
            all_of(in1.at[c], s1_sem, rf_sem.at[c]).wait_recv()
        for part in range(2):
            at = pl.multiple_of(me * tok_dev + part * half, 32)
            y = tok_all[c, pl.ds(at, half), :].astype(F32) + (
                own[c, part] + in1[c, part, 0].astype(F32) + in2[c, part].astype(F32))
            outv[c, part * half:(part + 1) * half, :] = y.astype(BF)
        out_copy(c).start()

    def second(c, _):
        for part in range(2):
            experts = range(part * (nexp // 2), (part + 1) * (nexp // 2))
            with NS('second'):
                wo_copy(c, part).wait()
            for e in experts:
                y = jnp.dot(hbf[e * cap:(e + 1) * cap, :], wo[part, e % nh], preferred_element_type=F32).astype(BF)
                obuf[e * (cap // 16):(e + 1) * (cap // 16)] = y.reshape(cap // 16, 16, wd)

            @pl.when(c + 1 < nch)
            def _():
                wo_copy(c + 1, part).start()

        for q, r in enumerate(RETURN_ORDER):
            hacc[c * 4 + q] = combine(r + 1)
        with NS('d2d'):
            for q in range(4):
                d2d_copy(c, q).start()
        for q, r in enumerate(RETURN_ORDER):
            mine[q] = combine(r)
        for q, r in enumerate(RETURN_ORDER):
            with NS('d2d_wait'):
                d2d_copy(c, q).wait_recv()
            y = mine[q] + d2d_in[c * 4 + q]
            if r == 6:
                out1[c, 0, 1] = y[:half].astype(BF)
                out1[c, 1, 1] = y[half:].astype(BF)
                hop1(c, 0, 1).start()
                hop1(c, 1, 1).start()
            elif r == 2:
                out1[c, 0, 0] = y[:half].astype(BF)
                kept[c, 1] = y[half:]
                hop1(c, 0, 0).start()
            elif r == 4:
                out1[c, 1, 0] = y[half:].astype(BF)
                kept[c, 0] = y[:half]
                hop1(c, 1, 0).start()
            else:
                own[c, 0] = y[:half]
                own[c, 1] = y[half:]

        @pl.when(c > 0)
        def _():
            relay(c - 1)

        @pl.when(c > 1)
        def _():
            finish(c - 2)
        return 0

    lax.fori_loop(0, nch, second, 0)
    relay(nch - 1)
    finish(nch - 2)
    finish(nch - 1)

    with NS('drain'):
        all_ids.wait_send()
        all_gates.wait_send()
        all_of(tok_all.at[:, 0:7 * tok_dev, :], as_sem, ar_sem.at[0, 0]).wait_send()
        all_of(hacc, ds_sem, dr_sem.at[0]).wait_send()
        all_of(out1, s1_sem, rf_sem.at[0]).wait_send()
        all_of(out2, s2_sem, rf_sem.at[0]).wait_send()
        for c in range(nch):
            out_copy(c).wait()


def solution(mesh):
    group_size = mesh.shape['row'] * mesh.shape['col']

    def device_fn(tokens, expert_ids, gate_weights, w_in, w_out):
        tok_dev, width = tokens.shape
        top_k = expert_ids.shape[1]
        nexp, _, ff = w_in.shape
        cap = tok_dev * group_size * top_k // (nexp * group_size)
        ntok = tok_dev * group_size
        nch = 4
        wd = width // nch
        half = tok_dev // 2
        dma = pltpu.SemaphoreType.DMA
        cfg = (tok_dev, cap, nexp, nch, wd, ff)
        hb = pl.BlockSpec(memory_space=pl.ANY)
        return pl.pallas_call(
            functools.partial(moe_kernel, cfg),
            out_shape=jax.ShapeDtypeStruct((tok_dev, width), BF),
            in_specs=[hb] * 5,
            out_specs=hb,
            scratch_shapes=[
                pltpu.VMEM((8, 8, 256), jnp.int32),
                pltpu.VMEM((8, 8, 256), F32),
                pltpu.VMEM((nch, ntok, wd), BF),
                pltpu.VMEM((nexp * cap, ntok), BF),
                pltpu.VMEM((3, ntok, nexp * WIN), BF),
                pltpu.VMEM((nexp * ff // wd, cap, wd), F32),
                pltpu.VMEM((nexp * cap, ff), BF),
                pltpu.VMEM((2, nexp // 2, wd, ff), BF),
                pltpu.VMEM((2, nexp // 2, ff, wd), BF),
                pltpu.VMEM((nexp * cap // 16, 16, wd), BF),
                pltpu.VMEM((nch * 4, tok_dev, wd), F32),
                pltpu.VMEM((nch, 2, 2, half, wd), BF),
                pltpu.VMEM((nch, 2, 2, half, wd), BF),
                pltpu.VMEM((nch, 2, half, wd), BF),
                pltpu.VMEM((nch, 2, half, wd), BF),
                pltpu.VMEM((nch, 2, half, wd), F32),
                pltpu.VMEM((nch, 2, half, wd), F32),
                pltpu.VMEM((4, tok_dev, wd), F32),
                pltpu.VMEM((nch, tok_dev, wd), BF),
                pltpu.VMEM((8, tok_dev), jnp.int32),
                pltpu.VMEM((8, tok_dev), F32),
                pltpu.VMEM((8, ntok), F32),
                pltpu.VMEM((ntok // 128, 32, 128), F32),
                pltpu.VMEM((8, 128), jnp.int32),
                pltpu.SMEM((8, 128), jnp.int32),
                dma((nch,)), dma((2,)), dma((2,)), dma, dma, dma, dma, dma, dma((nch, 5)), dma, dma((nch * 4,)),
                dma, dma((nch, 2)), dma, dma((nch,)), dma, dma((nch,)), dma, dma,
            ],
            compiler_params=pltpu.CompilerParams(collective_id=0, has_side_effects=True, vmem_limit_bytes=67000000),
        )(expert_ids.T, gate_weights.T, tokens, w_in, w_out)

    token_spec = P(('data', 'row', 'col'), None)
    expert_spec = P(GRID_AXES, None, None)
    return jax.shard_map(device_fn, mesh=mesh, in_specs=(token_spec, token_spec, token_spec, expert_spec, expert_spec),
                         out_specs=token_spec, check_vma=False)
```

```python
import functools

import jax
import jax.numpy as jnp
from jax import lax
from jax.experimental import pallas as pl
from jax.experimental.pallas import tpu as pltpu
from jax.sharding import PartitionSpec as P

NS = jax.named_scope
GRID_AXES = ('row', 'col')
MESH = pl.DeviceIdType.MESH
BF = jnp.bfloat16
F32 = jnp.float32
WIN = 64
LEAD = 2
AG_KINDS = ((0, None, 1), (0, None, 2), (0, None, 4), (2, 0, 4), (4, 1, 2), (2, None, 1), (4, None, 1), (6, 0, 1), (6, 1, 1))
RETURN_ORDER = (6, 2, 4, 0)


def moe_kernel(cfg, ids_hbm, gate_hbm, tok_hbm, wi_hbm, wo_hbm, out_hbm,
               ids_all, gate_all, tok_all, pmat, cmat, hacc, hbf, wi, wo, obuf, d2d_in, out1, in1, out2, in2, kept, own, mine, outv,
               ids_v, gate_v, slot_buf, zbuf, start_v, start_s,
               tok_sem, wi_sem, wo_sem, ms_sem, mr_sem, gs_sem, gr_sem, as_sem, ar_sem, ds_sem, dr_sem,
               s1_sem, r1_sem, s2_sem, rf_sem, st_sem, out_sem, id_sem, gate_sem):
    tok_dev, cap, nexp, nch, wd, ff = cfg
    ntok = 8 * tok_dev
    half = tok_dev // 2
    i = lax.axis_index('row')
    j = lax.axis_index('col')
    j_flip = j + 1 - 2 * lax.rem(j, 2)

    def rel(r):
        jj = j_flip if r & 1 else j
        if r & 2:
            jj = lax.rem(jj + 2, 4)
        ii = lax.rem(i + 1, 2) if r & 4 else i
        return ii, jj

    def dev(r):
        ii, jj = rel(r)
        return {'row': ii, 'col': jj}

    def gidx(r):
        ii, jj = rel(r)
        return ii * 4 + jj

    def rows_of(r):
        return pl.ds(pl.multiple_of(gidx(r) * tok_dev, 64), tok_dev)

    me = gidx(0)

    def tok_copy(c):
        return pltpu.make_async_copy(tok_hbm.at[:, pl.ds(c * wd, wd)], tok_all.at[c, rows_of(0), :], tok_sem.at[c])

    nh = nexp // 2

    def wi_copy(c, p):
        return pltpu.make_async_copy(wi_hbm.at[p * nh:(p + 1) * nh, pl.ds(c * wd, wd), :], wi.at[p], wi_sem.at[p])

    def wo_copy(c, p):
        return pltpu.make_async_copy(wo_hbm.at[p * nh:(p + 1) * nh, :, pl.ds(pl.multiple_of(c * wd, wd), wd)], wo.at[p],
                                     wo_sem.at[p])

    def out_copy(c):
        return pltpu.make_async_copy(outv.at[c], out_hbm.at[:, pl.ds(pl.multiple_of(c * wd, wd), wd)], out_sem.at[c])

    bar = pltpu.get_barrier_semaphore()
    for r in range(1, 8):
        pl.semaphore_signal(bar, inc=1, device_id=dev(r), device_id_type=MESH)
    ids_in = pltpu.make_async_copy(ids_hbm, ids_v, id_sem)
    gate_in = pltpu.make_async_copy(gate_hbm, gate_v, gate_sem)
    ids_in.start()
    gate_in.start()
    for c in range(nch):
        tok_copy(c).start()
    ids_all[me] = jnp.zeros((8, 256), jnp.int32)
    gate_all[me] = jnp.zeros((8, 256), F32)
    ids_in.wait()
    gate_in.wait()
    ids_all[me, :, :tok_dev] = ids_v[...]
    gate_all[me, :, :tok_dev] = gate_v[...]
    with NS('barrier'):
        pl.semaphore_wait(bar, 7)

    def ids_copy(r):
        return pltpu.make_async_remote_copy(ids_all.at[me], ids_all.at[me], ms_sem, mr_sem,
                                            device_id=dev(r), device_id_type=MESH)

    def gate_copy(r):
        return pltpu.make_async_remote_copy(gate_all.at[me], gate_all.at[me], gs_sem, gr_sem,
                                            device_id=dev(r), device_id_type=MESH)

    def ag_copy(c, kind, mine):
        owner, part, to = AG_KINDS[kind]
        if not mine:
            owner = owner ^ to
        start, size = gidx(owner) * tok_dev, tok_dev
        if part is not None:
            start, size = start + part * half, half
        ref = tok_all.at[c, pl.ds(pl.multiple_of(start, 32), size), :]
        return pltpu.make_async_remote_copy(ref, ref, as_sem, ar_sem.at[c, kind if kind in (1, 2, 3, 4) else 0],
                                            device_id=dev(to), device_id_type=MESH)

    def send_own(c):
        tok_copy(c).wait()
        for kind in (1, 2, 0):
            ag_copy(c, kind, True).start()

    def near(c):
        with NS('near_x'):
            ag_copy(c, 1, False).wait_recv()
        ag_copy(c, 3, True).start()
        ag_copy(c, 5, True).start()
        with NS('near_y'):
            ag_copy(c, 2, False).wait_recv()
        ag_copy(c, 4, True).start()
        ag_copy(c, 6, True).start()

    def far(c):
        with NS('far_a'):
            ag_copy(c, 3, False).wait_recv()
        ag_copy(c, 7, True).start()
        with NS('far_b'):
            ag_copy(c, 4, False).wait_recv()
        ag_copy(c, 8, True).start()

    for r in range(1, 8):
        ids_copy(r).start()
        gate_copy(r).start()
    for c in range(LEAD):
        send_own(c)
    for p in range(2):
        wi_copy(0, p).start()
    for p in range(2):
        wo_copy(0, p).start()

    def all_of(ref, send, recv):
        return pltpu.make_async_remote_copy(ref, ref, send, recv, device_id=dev(1), device_id_type=MESH)

    all_ids = all_of(ids_all.at[0:7], ms_sem, mr_sem)
    all_gates = all_of(gate_all.at[0:7], gs_sem, gr_sem)
    with NS('meta_wait'):
        all_ids.wait_recv()
        all_gates.wait_recv()

    lane = lax.broadcasted_iota(jnp.int32, (8, 128), 1)

    def compact(ref):
        out = []
        for m in range(4):
            a = ref[2 * m]
            b = pltpu.roll(ref[2 * m + 1], 64, 1)
            out += [a[:, :128], jnp.where(lane < 64, a[:, 128:], b[:, :128]), b[:, 128:]]
        return out

    id_blocks, gate_blocks = compact(ids_all), compact(gate_all)
    eid = lax.broadcasted_iota(jnp.int32, (8, 128), 0) + me * nexp
    imasks, gates = [], []
    for idb, gb in zip(id_blocks, gate_blocks):
        m = jnp.zeros((8, 128), jnp.int32)
        g = jnp.zeros((8, 128), F32)
        for k in range(8):
            hit = idb[k:k + 1, :] == eid
            m = jnp.where(hit, 1, m)
            g = jnp.where(hit, gb[k:k + 1, :], g)
        imasks.append(m)
        gates.append(g)
    masks = [m.astype(F32) for m in imasks]
    nb = len(masks)
    tri = jnp.where(lax.broadcasted_iota(jnp.int32, (128, 128), 0) < lax.broadcasted_iota(jnp.int32, (128, 128), 1),
                    1.0, 0.0).astype(BF)
    cums = jnp.dot(jnp.concatenate(masks, axis=0).astype(BF), tri, preferred_element_type=F32)
    carry = jnp.zeros((8, 1), F32)
    ranks = []
    for b in range(nb):
        ranks.append(cums[b * 8:b * 8 + 8, :] + carry)
        carry = carry + jnp.sum(masks[b], axis=1, keepdims=True)
    starts, seen = [], jnp.zeros((8, 128), jnp.int32)
    table = jnp.zeros((8, 128), jnp.int32)
    for g in range(8):
        b = 3 * (g // 2) + g % 2
        before = seen + jnp.where(lane < 64, imasks[b], 0) if g % 2 else seen
        off = jnp.sum(before, axis=1, keepdims=True)
        start16 = jnp.minimum(off >> 4, (cap - WIN) // 16)
        table = jnp.where(lane == g, start16, table)
        starts.append((start16 * 16).astype(F32))
        seen = seen + imasks[b]
        if g % 2:
            seen = seen + imasks[b + 1]
    start_v[...] = table
    st = pltpu.make_async_copy(start_v, start_s, st_sem)
    st.start()
    for b in range(nb):
        m = b // 3
        if b % 3 == 0:
            start = starts[2 * m]
        elif b % 3 == 1:
            start = jnp.where(lane < 64, starts[2 * m], starts[2 * m + 1])
        else:
            start = starts[2 * m + 1]
        keep = (masks[b] > 0.0) & (ranks[b] < float(cap))
        slot_buf[:, b * 128:(b + 1) * 128] = jnp.where(keep, ranks[b], -1.0)
        g1 = gates[b].astype(BF).astype(F32)
        rem1 = gates[b] - g1
        g2 = rem1.astype(BF).astype(F32)
        g3 = rem1 - g2
        zbuf[b, 0:8, :] = jnp.where(keep, ranks[b] - start, -1.0)
        zbuf[b, 8:16, :] = g1
        zbuf[b, 16:24, :] = g2
        zbuf[b, 24:32, :] = g3

    def build_p(e, _):
        row = slot_buf[pl.ds(e, 1), :]
        pos = lax.broadcasted_iota(jnp.int32, (cap, ntok), 0).astype(F32)
        pmat[pl.ds(pl.multiple_of(e * cap, 64), cap), :] = jnp.where(pos == row, 1.0, 0.0).astype(BF)
        return 0

    nwin = nexp * WIN

    def build_c(b, _):
        z = jnp.concatenate([zbuf[b], jnp.zeros((96, 128), F32)], axis=0)
        zt = jnp.transpose(z).astype(BF)
        ex = jnp.where(lax.broadcasted_iota(jnp.int32, (128, 4 * nwin), 0)
                       == lax.broadcasted_iota(jnp.int32, (128, 4 * nwin), 1) // WIN, 1.0, 0.0).astype(BF)
        y = jnp.dot(zt, ex, preferred_element_type=F32)
        wpos = lax.rem(lax.broadcasted_iota(jnp.int32, (128, nwin), 1), WIN).astype(F32)
        hit = y[:, :nwin] == wpos
        rows = pl.ds(pl.multiple_of(b * 128, 128), 128)
        for k in range(3):
            cmat[k, rows, :] = jnp.where(hit, y[:, (k + 1) * nwin:(k + 2) * nwin], 0.0).astype(BF)
        return 0

    def arrived(c):
        with NS('arrived'):
            all_of(tok_all.at[c, 0:4 * tok_dev, :], as_sem, ar_sem.at[c, 0]).wait_recv()

    def first(c, part):
        experts = range(part * (nexp // 2), (part + 1) * (nexp // 2))
        with NS('first'):
            wi_copy(c, part).wait()

        def dispatch(e):
            return jnp.dot(pmat[e * cap:(e + 1) * cap, :], tok_all[c], preferred_element_type=F32).astype(BF)

        def expand(e, rows):
            y = jnp.dot(rows, wi[part, e % nh], preferred_element_type=F32)
            for n in range(ff // wd):
                yn = y[:, n * wd:(n + 1) * wd]
                if c:
                    yn = yn + hacc[e * (ff // wd) + n]
                if c == nch - 1:
                    hbf[e * cap:(e + 1) * cap, n * wd:(n + 1) * wd] = jax.nn.gelu(yn, approximate=True).astype(BF)
                else:
                    hacc[e * (ff // wd) + n] = yn

        ready = None
        for e in experts:
            rows = dispatch(e)
            if ready is not None:
                expand(*ready)
            ready = (e, rows)
        expand(*ready)
        if c + 1 < nch:
            wi_copy(c + 1, part).start()

    with NS('build_p'):
        lax.fori_loop(0, nexp, build_p, 0)
    near(0)
    send_own(2)
    with NS('build_c'):
        lax.fori_loop(0, nb // 2, build_c, 0)
    near(1)
    send_own(3)
    with NS('build_c'):
        lax.fori_loop(nb // 2, nb, build_c, 0)
    far(0)
    arrived(0)
    first(0, 0)
    first(0, 1)
    near(2)
    far(1)
    arrived(1)
    first(1, 0)
    near(3)
    first(1, 1)
    far(2)
    arrived(2)
    first(2, 0)
    far(3)
    first(2, 1)
    arrived(3)
    first(3, 0)
    first(3, 1)
    st.wait()

    def d2d_copy(c, q):
        k = c * 4 + q
        return pltpu.make_async_remote_copy(hacc.at[k], d2d_in.at[k], ds_sem, dr_sem.at[k],
                                            device_id=dev(1), device_id_type=MESH)

    def hop1(c, axis, k):
        recv = r1_sem.at[c, axis] if k else rf_sem.at[c]
        return pltpu.make_async_remote_copy(out1.at[c, axis, k], in1.at[c, axis, k], s1_sem, recv,
                                            device_id=dev(4 if axis else 2), device_id_type=MESH)

    def hop2(c, part):
        return pltpu.make_async_remote_copy(out2.at[c, part], in2.at[c, part], s2_sem, rf_sem.at[c],
                                            device_id=dev(2 if part else 4), device_id_type=MESH)

    def combine(r):
        g = gidx(r)
        parts = []
        for e in range(nexp):
            at = e * (cap // 16) + start_s[e, g]
            parts.append(obuf[pl.ds(at, WIN // 16)].reshape(WIN, wd))
        win = jnp.concatenate(parts, axis=0)
        rows = pl.ds(pl.multiple_of(g * tok_dev, 64), tok_dev)
        lhs = jnp.concatenate([cmat[k, rows, :] for k in range(3)], axis=0)
        y = jnp.dot(lhs, win, preferred_element_type=F32)
        return y[:tok_dev] + y[tok_dev:2 * tok_dev] + y[2 * tok_dev:]

    def relay(c):
        for part in range(2):
            with NS('relay'):
                hop1(c, part, 1).wait_recv()
            out2[c, part] = (kept[c, part] + in1[c, part, 1].astype(F32)).astype(BF)
            hop2(c, part).start()

    def finish(c):
        with NS('finish'):
            all_of(in1.at[c], s1_sem, rf_sem.at[c]).wait_recv()
        for part in range(2):
            at = pl.multiple_of(me * tok_dev + part * half, 32)
            y = tok_all[c, pl.ds(at, half), :].astype(F32) + (
                own[c, part] + in1[c, part, 0].astype(F32) + in2[c, part].astype(F32))
            outv[c, part * half:(part + 1) * half, :] = y.astype(BF)
        out_copy(c).start()

    def second(c, _):
        for part in range(2):
            experts = range(part * (nexp // 2), (part + 1) * (nexp // 2))
            with NS('second'):
                wo_copy(c, part).wait()
            for e in experts:
                y = jnp.dot(hbf[e * cap:(e + 1) * cap, :], wo[part, e % nh], preferred_element_type=F32).astype(BF)
                obuf[e * (cap // 16):(e + 1) * (cap // 16)] = y.reshape(cap // 16, 16, wd)

            @pl.when(c + 1 < nch)
            def _():
                wo_copy(c + 1, part).start()

        for pair in ((0, 1), (2, 3)):
            for q in pair:
                hacc[c * 4 + q] = combine(RETURN_ORDER[q] + 1)
            with NS('d2d'):
                for q in pair:
                    d2d_copy(c, q).start()
        for q in (0, 1):
            mine[q] = combine(RETURN_ORDER[q])
        for q, r in enumerate(RETURN_ORDER):
            if q == 2:
                for k in (2, 3):
                    mine[k] = combine(RETURN_ORDER[k])
            with NS('d2d_wait'):
                d2d_copy(c, q).wait_recv()
            y = mine[q] + d2d_in[c * 4 + q]
            if r == 6:
                out1[c, 0, 1] = y[:half].astype(BF)
                out1[c, 1, 1] = y[half:].astype(BF)
                hop1(c, 0, 1).start()
                hop1(c, 1, 1).start()
            elif r == 2:
                out1[c, 0, 0] = y[:half].astype(BF)
                kept[c, 1] = y[half:]
                hop1(c, 0, 0).start()
            elif r == 4:
                out1[c, 1, 0] = y[half:].astype(BF)
                kept[c, 0] = y[:half]
                hop1(c, 1, 0).start()
            else:
                own[c, 0] = y[:half]
                own[c, 1] = y[half:]

        @pl.when(c > 0)
        def _():
            relay(c - 1)

        @pl.when(c > 1)
        def _():
            finish(c - 2)
        return 0

    lax.fori_loop(0, nch, second, 0)
    relay(nch - 1)
    finish(nch - 2)
    finish(nch - 1)

    with NS('drain'):
        all_ids.wait_send()
        all_gates.wait_send()
        all_of(tok_all.at[:, 0:7 * tok_dev, :], as_sem, ar_sem.at[0, 0]).wait_send()
        all_of(hacc, ds_sem, dr_sem.at[0]).wait_send()
        all_of(out1, s1_sem, rf_sem.at[0]).wait_send()
        all_of(out2, s2_sem, rf_sem.at[0]).wait_send()
        for c in range(nch):
            out_copy(c).wait()


def solution(mesh):
    group_size = mesh.shape['row'] * mesh.shape['col']

    def device_fn(tokens, expert_ids, gate_weights, w_in, w_out):
        tok_dev, width = tokens.shape
        top_k = expert_ids.shape[1]
        nexp, _, ff = w_in.shape
        cap = tok_dev * group_size * top_k // (nexp * group_size)
        ntok = tok_dev * group_size
        nch = 4
        wd = width // nch
        half = tok_dev // 2
        dma = pltpu.SemaphoreType.DMA
        cfg = (tok_dev, cap, nexp, nch, wd, ff)
        hb = pl.BlockSpec(memory_space=pl.ANY)
        return pl.pallas_call(
            functools.partial(moe_kernel, cfg),
            out_shape=jax.ShapeDtypeStruct((tok_dev, width), BF),
            in_specs=[hb] * 5,
            out_specs=hb,
            scratch_shapes=[
                pltpu.VMEM((8, 8, 256), jnp.int32),
                pltpu.VMEM((8, 8, 256), F32),
                pltpu.VMEM((nch, ntok, wd), BF),
                pltpu.VMEM((nexp * cap, ntok), BF),
                pltpu.VMEM((3, ntok, nexp * WIN), BF),
                pltpu.VMEM((nexp * ff // wd, cap, wd), F32),
                pltpu.VMEM((nexp * cap, ff), BF),
                pltpu.VMEM((2, nexp // 2, wd, ff), BF),
                pltpu.VMEM((2, nexp // 2, ff, wd), BF),
                pltpu.VMEM((nexp * cap // 16, 16, wd), BF),
                pltpu.VMEM((nch * 4, tok_dev, wd), F32),
                pltpu.VMEM((nch, 2, 2, half, wd), BF),
                pltpu.VMEM((nch, 2, 2, half, wd), BF),
                pltpu.VMEM((nch, 2, half, wd), BF),
                pltpu.VMEM((nch, 2, half, wd), BF),
                pltpu.VMEM((nch, 2, half, wd), F32),
                pltpu.VMEM((nch, 2, half, wd), F32),
                pltpu.VMEM((4, tok_dev, wd), F32),
                pltpu.VMEM((nch, tok_dev, wd), BF),
                pltpu.VMEM((8, tok_dev), jnp.int32),
                pltpu.VMEM((8, tok_dev), F32),
                pltpu.VMEM((8, ntok), F32),
                pltpu.VMEM((ntok // 128, 32, 128), F32),
                pltpu.VMEM((8, 128), jnp.int32),
                pltpu.SMEM((8, 128), jnp.int32),
                dma((nch,)), dma((2,)), dma((2,)), dma, dma, dma, dma, dma, dma((nch, 5)), dma, dma((nch * 4,)),
                dma, dma((nch, 2)), dma, dma((nch,)), dma, dma((nch,)), dma, dma,
            ],
            compiler_params=pltpu.CompilerParams(collective_id=0, has_side_effects=True, vmem_limit_bytes=67000000),
        )(expert_ids.T, gate_weights.T, tokens, w_in, w_out)

    token_spec = P(('data', 'row', 'col'), None)
    expert_spec = P(GRID_AXES, None, None)
    return jax.shard_map(device_fn, mesh=mesh, in_specs=(token_spec, token_spec, token_spec, expert_spec, expert_spec),
                         out_specs=token_spec, check_vma=False)
```

```python
import functools
import math

import jax
import jax.numpy as jnp
from jax import lax
from jax.experimental import pallas as pl
from jax.experimental.pallas import tpu as pltpu
from jax.sharding import PartitionSpec as P

GRID_AXES = ('row', 'col')
MESH = pl.DeviceIdType.MESH
BF = jnp.bfloat16
F32 = jnp.float32
WIN = 64
LEAD = 2
AG_KINDS = ((0, None, 1), (0, None, 2), (0, None, 4), (2, 0, 4), (4, 1, 2), (2, None, 1), (4, None, 1), (6, 0, 1), (6, 1, 1))
RETURN_ORDER = (6, 2, 4, 0)


def gelu_tanh(x):
    scale = (2.0 / math.pi) ** 0.5
    h = 0.5 * x
    return h + h * jnp.tanh(x * (scale + (scale * 0.044715) * (x * x)))


def moe_kernel(cfg, ids_hbm, gate_hbm, tok_hbm, wi_hbm, wo_hbm, out_hbm,
               ids_all, gate_all, tok_all, pmat, cmat, hacc, hbf, wi, wo, obuf, d2d_out, d2d_in, out1, in1, out2, in2, kept, own, outv,
               ids_v, gate_v, slot_buf, zbuf, start_v, start_s,
               tok_sem, wi_sem, wo_sem, ms_sem, mr_sem, gs_sem, gr_sem, as_sem, ar_sem, ds_sem, dr_sem,
               s1_sem, r1_sem, s2_sem, rf_sem, st_sem, out_sem, id_sem, gate_sem):
    tok_dev, cap, nexp, nch, wd, ff = cfg
    ntok = 8 * tok_dev
    half = tok_dev // 2
    i = lax.axis_index('row')
    j = lax.axis_index('col')
    j_flip = j + 1 - 2 * lax.rem(j, 2)

    def rel(r):
        jj = j_flip if r & 1 else j
        if r & 2:
            jj = lax.rem(jj + 2, 4)
        ii = lax.rem(i + 1, 2) if r & 4 else i
        return ii, jj

    def dev(r):
        ii, jj = rel(r)
        return {'row': ii, 'col': jj}

    def gidx(r):
        ii, jj = rel(r)
        return ii * 4 + jj

    def rows_of(r):
        return pl.ds(pl.multiple_of(gidx(r) * tok_dev, 64), tok_dev)

    me = gidx(0)

    def tok_copy(c):
        return pltpu.make_async_copy(tok_hbm.at[:, pl.ds(c * wd, wd)], tok_all.at[c, rows_of(0), :], tok_sem.at[c])

    nh = nexp // 2

    def wi_copy(c, p):
        return pltpu.make_async_copy(wi_hbm.at[p * nh:(p + 1) * nh, pl.ds(c * wd, wd), :], wi.at[p], wi_sem.at[p])

    def wo_copy(c, p):
        return pltpu.make_async_copy(wo_hbm.at[p * nh:(p + 1) * nh, :, pl.ds(pl.multiple_of(c * wd, wd), wd)], wo.at[p],
                                     wo_sem.at[p])

    def out_copy(c):
        return pltpu.make_async_copy(outv.at[c], out_hbm.at[:, pl.ds(pl.multiple_of(c * wd, wd), wd)], out_sem.at[c])

    bar = pltpu.get_barrier_semaphore()
    for r in range(1, 8):
        pl.semaphore_signal(bar, inc=1, device_id=dev(r), device_id_type=MESH)
    ids_in = pltpu.make_async_copy(ids_hbm, ids_v, id_sem)
    gate_in = pltpu.make_async_copy(gate_hbm, gate_v, gate_sem)
    ids_in.start()
    gate_in.start()
    for c in range(nch):
        tok_copy(c).start()
    ids_all[me] = jnp.zeros((8, 256), jnp.int32)
    gate_all[me] = jnp.zeros((8, 256), F32)
    ids_in.wait()
    gate_in.wait()
    ids_all[me, :, :tok_dev] = ids_v[...]
    gate_all[me, :, :tok_dev] = gate_v[...]
    pl.semaphore_wait(bar, 7)

    def ids_copy(r):
        return pltpu.make_async_remote_copy(ids_all.at[me], ids_all.at[me], ms_sem, mr_sem,
                                            device_id=dev(r), device_id_type=MESH)

    def gate_copy(r):
        return pltpu.make_async_remote_copy(gate_all.at[me], gate_all.at[me], gs_sem, gr_sem,
                                            device_id=dev(r), device_id_type=MESH)

    def ag_copy(c, kind, mine):
        owner, part, to = AG_KINDS[kind]
        if not mine:
            owner = owner ^ to
        start, size = gidx(owner) * tok_dev, tok_dev
        if part is not None:
            start, size = start + part * half, half
        ref = tok_all.at[c, pl.ds(pl.multiple_of(start, 32), size), :]
        return pltpu.make_async_remote_copy(ref, ref, as_sem, ar_sem.at[c, kind if kind in (1, 2, 3, 4) else 0],
                                            device_id=dev(to), device_id_type=MESH)

    def send_own(c):
        tok_copy(c).wait()
        for kind in (1, 2, 0):
            ag_copy(c, kind, True).start()

    def near(c):
        ag_copy(c, 1, False).wait_recv()
        ag_copy(c, 3, True).start()
        ag_copy(c, 5, True).start()
        ag_copy(c, 2, False).wait_recv()
        ag_copy(c, 4, True).start()
        ag_copy(c, 6, True).start()

    def far(c):
        ag_copy(c, 3, False).wait_recv()
        ag_copy(c, 7, True).start()
        ag_copy(c, 4, False).wait_recv()
        ag_copy(c, 8, True).start()

    for r in range(1, 8):
        ids_copy(r).start()
        gate_copy(r).start()
    for c in range(LEAD):
        send_own(c)
    for p in range(2):
        wi_copy(0, p).start()
    for p in range(2):
        wo_copy(0, p).start()

    def all_of(ref, send, recv):
        return pltpu.make_async_remote_copy(ref, ref, send, recv, device_id=dev(1), device_id_type=MESH)

    all_ids = all_of(ids_all.at[0:7], ms_sem, mr_sem)
    all_gates = all_of(gate_all.at[0:7], gs_sem, gr_sem)
    all_ids.wait_recv()
    all_gates.wait_recv()

    lane = lax.broadcasted_iota(jnp.int32, (8, 128), 1)

    def compact(ref):
        out = []
        for m in range(4):
            a = ref[2 * m]
            b = pltpu.roll(ref[2 * m + 1], 64, 1)
            out += [a[:, :128], jnp.where(lane < 64, a[:, 128:], b[:, :128]), b[:, 128:]]
        return out

    id_blocks, gate_blocks = compact(ids_all), compact(gate_all)
    eid = lax.broadcasted_iota(jnp.int32, (8, 128), 0) + me * nexp
    imasks, gates = [], []
    for idb, gb in zip(id_blocks, gate_blocks):
        m = jnp.zeros((8, 128), jnp.int32)
        g = jnp.zeros((8, 128), F32)
        for k in range(8):
            hit = idb[k:k + 1, :] == eid
            m = jnp.where(hit, 1, m)
            g = jnp.where(hit, gb[k:k + 1, :], g)
        imasks.append(m)
        gates.append(g)
    masks = [m.astype(F32) for m in imasks]
    nb = len(masks)
    tri = jnp.where(lax.broadcasted_iota(jnp.int32, (128, 128), 0) < lax.broadcasted_iota(jnp.int32, (128, 128), 1),
                    1.0, 0.0).astype(BF)
    cums = jnp.dot(jnp.concatenate(masks, axis=0).astype(BF), tri, preferred_element_type=F32)
    carry = jnp.zeros((8, 1), F32)
    ranks = []
    for b in range(nb):
        ranks.append(cums[b * 8:b * 8 + 8, :] + carry)
        carry = carry + jnp.sum(masks[b], axis=1, keepdims=True)
    starts, seen = [], jnp.zeros((8, 128), jnp.int32)
    table = jnp.zeros((8, 128), jnp.int32)
    for g in range(8):
        b = 3 * (g // 2) + g % 2
        before = seen + jnp.where(lane < 64, imasks[b], 0) if g % 2 else seen
        off = jnp.sum(before, axis=1, keepdims=True)
        start16 = jnp.minimum(off >> 4, (cap - WIN) // 16)
        table = jnp.where(lane == g, start16, table)
        starts.append((start16 * 16).astype(F32))
        seen = seen + imasks[b]
        if g % 2:
            seen = seen + imasks[b + 1]
    start_v[...] = table
    st = pltpu.make_async_copy(start_v, start_s, st_sem)
    st.start()
    for b in range(nb):
        m = b // 3
        if b % 3 == 0:
            start = starts[2 * m]
        elif b % 3 == 1:
            start = jnp.where(lane < 64, starts[2 * m], starts[2 * m + 1])
        else:
            start = starts[2 * m + 1]
        keep = (masks[b] > 0.0) & (ranks[b] < float(cap))
        slot_buf[:, b * 128:(b + 1) * 128] = jnp.where(keep, ranks[b], -1.0)
        g1 = gates[b].astype(BF).astype(F32)
        rem1 = gates[b] - g1
        g2 = rem1.astype(BF).astype(F32)
        g3 = rem1 - g2
        zbuf[b, 0:8, :] = jnp.where(keep, ranks[b] - start, -1.0)
        zbuf[b, 8:16, :] = g1
        zbuf[b, 16:24, :] = g2
        zbuf[b, 24:32, :] = g3

    def build_p(e, _):
        row = slot_buf[pl.ds(e, 1), :]
        pos = lax.broadcasted_iota(jnp.int32, (cap, ntok), 0).astype(F32)
        pmat[pl.ds(pl.multiple_of(e * cap, 64), cap), :] = jnp.where(pos == row, 1.0, 0.0).astype(BF)
        return 0

    nwin = nexp * WIN

    def build_c(b, _):
        z = jnp.concatenate([zbuf[b], jnp.zeros((96, 128), F32)], axis=0)
        zt = jnp.transpose(z).astype(BF)
        ex = jnp.where(lax.broadcasted_iota(jnp.int32, (128, 4 * nwin), 0)
                       == lax.broadcasted_iota(jnp.int32, (128, 4 * nwin), 1) // WIN, 1.0, 0.0).astype(BF)
        y = jnp.dot(zt, ex, preferred_element_type=F32)
        wpos = lax.rem(lax.broadcasted_iota(jnp.int32, (128, nwin), 1), WIN).astype(F32)
        hit = y[:, :nwin] == wpos
        rows = pl.ds(pl.multiple_of(b * 128, 128), 128)
        for k in range(3):
            cmat[k, rows, :] = jnp.where(hit, y[:, (k + 1) * nwin:(k + 2) * nwin], 0.0).astype(BF)
        return 0

    def arrived(c):
        all_of(tok_all.at[c, 0:4 * tok_dev, :], as_sem, ar_sem.at[c, 0]).wait_recv()

    def first(c, part):
        experts = range(part * (nexp // 2), (part + 1) * (nexp // 2))
        wi_copy(c, part).wait()

        def dispatch(e):
            return jnp.dot(pmat[e * cap:(e + 1) * cap, :], tok_all[c], preferred_element_type=F32).astype(BF)

        def expand(e, rows):
            y = jnp.dot(rows, wi[part, e % nh], preferred_element_type=F32)
            for n in range(ff // wd):
                yn = y[:, n * wd:(n + 1) * wd]
                if c:
                    yn = yn + hacc[e * (ff // wd) + n]
                if c == nch - 1:
                    hbf[e * cap:(e + 1) * cap, n * wd:(n + 1) * wd] = gelu_tanh(yn).astype(BF)
                else:
                    hacc[e * (ff // wd) + n] = yn

        ready = None
        for e in experts:
            rows = dispatch(e)
            if ready is not None:
                expand(*ready)
            ready = (e, rows)
        expand(*ready)
        if c + 1 < nch:
            wi_copy(c + 1, part).start()

    lax.fori_loop(0, nexp, build_p, 0)
    near(0)
    send_own(2)
    lax.fori_loop(0, nb // 2, build_c, 0)
    near(1)
    send_own(3)
    lax.fori_loop(nb // 2, nb, build_c, 0)
    far(0)
    arrived(0)
    first(0, 0)
    first(0, 1)
    near(2)
    far(1)
    arrived(1)
    first(1, 0)
    near(3)
    first(1, 1)
    far(2)
    arrived(2)
    first(2, 0)
    far(3)
    first(2, 1)
    arrived(3)
    first(3, 0)
    first(3, 1)
    st.wait()

    def d2d_copy(c, q):
        k = c * 4 + q
        return pltpu.make_async_remote_copy(d2d_out.at[k], d2d_in.at[k], ds_sem, dr_sem.at[k],
                                            device_id=dev(1), device_id_type=MESH)

    def hop1(c, axis, k):
        recv = r1_sem.at[c, axis] if k else rf_sem.at[c]
        return pltpu.make_async_remote_copy(out1.at[c, axis, k], in1.at[c, axis, k], s1_sem, recv,
                                            device_id=dev(4 if axis else 2), device_id_type=MESH)

    def hop2(c, part):
        return pltpu.make_async_remote_copy(out2.at[c, part], in2.at[c, part], s2_sem, rf_sem.at[c],
                                            device_id=dev(2 if part else 4), device_id_type=MESH)

    def combine(r):
        g = gidx(r)
        parts = []
        for e in range(nexp):
            at = e * (cap // 16) + start_s[e, g]
            parts.append(obuf[pl.ds(at, WIN // 16)].reshape(WIN, wd))
        win = jnp.concatenate(parts, axis=0)
        rows = pl.ds(pl.multiple_of(g * tok_dev, 64), tok_dev)
        lhs = jnp.concatenate([cmat[k, rows, :] for k in range(3)], axis=0)
        y = jnp.dot(lhs, win, preferred_element_type=F32)
        return y[:tok_dev] + y[tok_dev:2 * tok_dev] + y[2 * tok_dev:]

    def relay(c):
        for part in range(2):
            hop1(c, part, 1).wait_recv()
            out2[c, part] = (kept[c, part] + in1[c, part, 1].astype(F32)).astype(BF)
            hop2(c, part).start()

    def finish(c):
        all_of(in1.at[c], s1_sem, rf_sem.at[c]).wait_recv()
        for part in range(2):
            at = pl.multiple_of(me * tok_dev + part * half, 32)
            y = tok_all[c, pl.ds(at, half), :].astype(F32) + (
                own[c, part] + in1[c, part, 0].astype(F32) + in2[c, part].astype(F32))
            outv[c, part * half:(part + 1) * half, :] = y.astype(BF)
        out_copy(c).start()

    def second(c, _):
        for part in range(2):
            experts = range(part * (nexp // 2), (part + 1) * (nexp // 2))
            wo_copy(c, part).wait()
            for e in experts:
                y = jnp.dot(hbf[e * cap:(e + 1) * cap, :], wo[part, e % nh], preferred_element_type=F32).astype(BF)
                obuf[e * (cap // 16):(e + 1) * (cap // 16)] = y.reshape(cap // 16, 16, wd)

            @pl.when(c + 1 < nch)
            def _():
                wo_copy(c + 1, part).start()

        for pair in ((0, 1), (2, 3)):
            for q in pair:
                d2d_out[c * 4 + q] = combine(RETURN_ORDER[q] + 1).astype(BF)
            for q in pair:
                d2d_copy(c, q).start()
        for q in (0, 1):
            hacc[q] = combine(RETURN_ORDER[q])
        for q, r in enumerate(RETURN_ORDER):
            if q == 2:
                for k in (2, 3):
                    hacc[k] = combine(RETURN_ORDER[k])
            d2d_copy(c, q).wait_recv()
            y = hacc[q] + d2d_in[c * 4 + q].astype(F32)
            if r == 6:
                out1[c, 0, 1] = y[:half].astype(BF)
                out1[c, 1, 1] = y[half:].astype(BF)
                hop1(c, 0, 1).start()
                hop1(c, 1, 1).start()
            elif r == 2:
                out1[c, 0, 0] = y[:half].astype(BF)
                kept[c, 1] = y[half:]
                hop1(c, 0, 0).start()
            elif r == 4:
                out1[c, 1, 0] = y[half:].astype(BF)
                kept[c, 0] = y[:half]
                hop1(c, 1, 0).start()
            else:
                own[c, 0] = y[:half]
                own[c, 1] = y[half:]

        @pl.when(c > 0)
        def _():
            relay(c - 1)

        @pl.when(c > 1)
        def _():
            finish(c - 2)
        return 0

    lax.fori_loop(0, nch, second, 0)
    relay(nch - 1)
    finish(nch - 2)
    finish(nch - 1)

    all_ids.wait_send()
    all_gates.wait_send()
    all_of(tok_all.at[:, 0:7 * tok_dev, :], as_sem, ar_sem.at[0, 0]).wait_send()
    all_of(d2d_out, ds_sem, dr_sem.at[0]).wait_send()
    all_of(out1, s1_sem, rf_sem.at[0]).wait_send()
    all_of(out2, s2_sem, rf_sem.at[0]).wait_send()
    for c in range(nch):
        out_copy(c).wait()


def solution(mesh):
    group_size = mesh.shape['row'] * mesh.shape['col']

    def device_fn(tokens, expert_ids, gate_weights, w_in, w_out):
        tok_dev, width = tokens.shape
        top_k = expert_ids.shape[1]
        nexp, _, ff = w_in.shape
        cap = tok_dev * group_size * top_k // (nexp * group_size)
        ntok = tok_dev * group_size
        nch = 4
        wd = width // nch
        half = tok_dev // 2
        dma = pltpu.SemaphoreType.DMA
        cfg = (tok_dev, cap, nexp, nch, wd, ff)
        hb = pl.BlockSpec(memory_space=pl.ANY)
        return pl.pallas_call(
            functools.partial(moe_kernel, cfg),
            out_shape=jax.ShapeDtypeStruct((tok_dev, width), BF),
            in_specs=[hb] * 5,
            out_specs=hb,
            scratch_shapes=[
                pltpu.VMEM((8, 8, 256), jnp.int32),
                pltpu.VMEM((8, 8, 256), F32),
                pltpu.VMEM((nch, ntok, wd), BF),
                pltpu.VMEM((nexp * cap, ntok), BF),
                pltpu.VMEM((3, ntok, nexp * WIN), BF),
                pltpu.VMEM((nexp * ff // wd, cap, wd), F32),
                pltpu.VMEM((nexp * cap, ff), BF),
                pltpu.VMEM((2, nexp // 2, wd, ff), BF),
                pltpu.VMEM((2, nexp // 2, ff, wd), BF),
                pltpu.VMEM((nexp * cap // 16, 16, wd), BF),
                pltpu.VMEM((nch * 4, tok_dev, wd), BF),
                pltpu.VMEM((nch * 4, tok_dev, wd), BF),
                pltpu.VMEM((nch, 2, 2, half, wd), BF),
                pltpu.VMEM((nch, 2, 2, half, wd), BF),
                pltpu.VMEM((nch, 2, half, wd), BF),
                pltpu.VMEM((nch, 2, half, wd), BF),
                pltpu.VMEM((nch, 2, half, wd), F32),
                pltpu.VMEM((nch, 2, half, wd), F32),
                pltpu.VMEM((nch, tok_dev, wd), BF),
                pltpu.VMEM((8, tok_dev), jnp.int32),
                pltpu.VMEM((8, tok_dev), F32),
                pltpu.VMEM((8, ntok), F32),
                pltpu.VMEM((ntok // 128, 32, 128), F32),
                pltpu.VMEM((8, 128), jnp.int32),
                pltpu.SMEM((8, 128), jnp.int32),
                dma((nch,)), dma((2,)), dma((2,)), dma, dma, dma, dma, dma, dma((nch, 5)), dma, dma((nch * 4,)),
                dma, dma((nch, 2)), dma, dma((nch,)), dma, dma((nch,)), dma, dma,
            ],
            compiler_params=pltpu.CompilerParams(collective_id=0, has_side_effects=True, vmem_limit_bytes=67000000),
        )(expert_ids.T, gate_weights.T, tokens, w_in, w_out)

    token_spec = P(('data', 'row', 'col'), None)
    expert_spec = P(GRID_AXES, None, None)
    return jax.shard_map(device_fn, mesh=mesh, in_specs=(token_spec, token_spec, token_spec, expert_spec, expert_spec),
                         out_specs=token_spec, check_vma=False)
```

```python
import functools
import math

import jax
import jax.numpy as jnp
from jax import lax
from jax.experimental import pallas as pl
from jax.experimental.pallas import tpu as pltpu
from jax.sharding import PartitionSpec as P

GRID_AXES = ('row', 'col')
MESH = pl.DeviceIdType.MESH
BF = jnp.bfloat16
F32 = jnp.float32
WIN = 64
LEAD = 2
AG_KINDS = ((0, None, 1), (0, None, 2), (0, None, 4), (2, 0, 4), (4, 1, 2), (2, None, 1), (4, None, 1), (6, 0, 1), (6, 1, 1))
RETURN_ORDER = (6, 2, 4, 0)


def gelu_tanh(x):
    scale = (2.0 / math.pi) ** 0.5
    h = 0.5 * x
    return h + h * jnp.tanh(x * (scale + (scale * 0.044715) * (x * x)))


def moe_kernel(cfg, ids_hbm, gate_hbm, tok_hbm, wi_hbm, wo_hbm, out_hbm,
               ids_all, gate_all, tok_all, pmat, cmat, hacc, hbf, wi, wo, obuf, d2d_out, d2d_in, out1, in1, out2, in2, kept, own,
               ids_v, gate_v, slot_buf, zbuf, start_v, start_s,
               tok_sem, wi_sem, wo_sem, ms_sem, mr_sem, gs_sem, gr_sem, as_sem, ar_sem, ds_sem, dr_sem,
               s1_sem, r1_sem, s2_sem, rf_sem, st_sem, out_sem, id_sem, gate_sem):
    tok_dev, cap, nexp, nch, wd, ff = cfg
    ntok = 8 * tok_dev
    half = tok_dev // 2
    i = lax.axis_index('row')
    j = lax.axis_index('col')
    j_flip = j + 1 - 2 * lax.rem(j, 2)

    def rel(r):
        jj = j_flip if r & 1 else j
        if r & 2:
            jj = lax.rem(jj + 2, 4)
        ii = lax.rem(i + 1, 2) if r & 4 else i
        return ii, jj

    def dev(r):
        ii, jj = rel(r)
        return {'row': ii, 'col': jj}

    def gidx(r):
        ii, jj = rel(r)
        return ii * 4 + jj

    def rows_of(r):
        return pl.ds(pl.multiple_of(gidx(r) * tok_dev, 64), tok_dev)

    me = gidx(0)

    def tok_copy(c):
        return pltpu.make_async_copy(tok_hbm.at[:, pl.ds(c * wd, wd)], tok_all.at[c, rows_of(0), :], tok_sem.at[c])

    nh = nexp // 2

    def wi_copy(c, p):
        return pltpu.make_async_copy(wi_hbm.at[p * nh:(p + 1) * nh, pl.ds(c * wd, wd), :], wi.at[p], wi_sem.at[p])

    def wo_copy(c, p):
        return pltpu.make_async_copy(wo_hbm.at[p * nh:(p + 1) * nh, :, pl.ds(pl.multiple_of(c * wd, wd), wd)], wo.at[p],
                                     wo_sem.at[p])

    def out_copy(c):
        return pltpu.make_async_copy(own.at[c], out_hbm.at[:, :, pl.ds(pl.multiple_of(c * wd, wd), wd)], out_sem.at[c])

    bar = pltpu.get_barrier_semaphore()
    for r in range(1, 8):
        pl.semaphore_signal(bar, inc=1, device_id=dev(r), device_id_type=MESH)
    ids_in = pltpu.make_async_copy(ids_hbm, ids_v, id_sem)
    gate_in = pltpu.make_async_copy(gate_hbm, gate_v, gate_sem)
    ids_in.start()
    gate_in.start()
    for c in range(nch):
        tok_copy(c).start()
    ids_all[me] = jnp.zeros((8, 256), jnp.int32)
    gate_all[me] = jnp.zeros((8, 256), F32)
    ids_in.wait()
    gate_in.wait()
    ids_all[me, :, :tok_dev] = ids_v[...]
    gate_all[me, :, :tok_dev] = gate_v[...]
    pl.semaphore_wait(bar, 7)

    def ids_copy(r):
        return pltpu.make_async_remote_copy(ids_all.at[me], ids_all.at[me], ms_sem, mr_sem,
                                            device_id=dev(r), device_id_type=MESH)

    def gate_copy(r):
        return pltpu.make_async_remote_copy(gate_all.at[me], gate_all.at[me], gs_sem, gr_sem,
                                            device_id=dev(r), device_id_type=MESH)

    def ag_copy(c, kind, mine):
        owner, part, to = AG_KINDS[kind]
        if not mine:
            owner = owner ^ to
        start, size = gidx(owner) * tok_dev, tok_dev
        if part is not None:
            start, size = start + part * half, half
        ref = tok_all.at[c, pl.ds(pl.multiple_of(start, 32), size), :]
        return pltpu.make_async_remote_copy(ref, ref, as_sem, ar_sem.at[c, kind if kind in (1, 2, 3, 4) else 0],
                                            device_id=dev(to), device_id_type=MESH)

    def send_own(c):
        tok_copy(c).wait()
        for kind in (1, 2, 0):
            ag_copy(c, kind, True).start()

    def near(c):
        ag_copy(c, 1, False).wait_recv()
        ag_copy(c, 3, True).start()
        ag_copy(c, 5, True).start()
        ag_copy(c, 2, False).wait_recv()
        ag_copy(c, 4, True).start()
        ag_copy(c, 6, True).start()

    def far(c):
        ag_copy(c, 3, False).wait_recv()
        ag_copy(c, 7, True).start()
        ag_copy(c, 4, False).wait_recv()
        ag_copy(c, 8, True).start()

    for r in range(1, 8):
        ids_copy(r).start()
        gate_copy(r).start()
    for c in range(LEAD):
        send_own(c)
    for p in range(2):
        wi_copy(0, p).start()
    for p in range(2):
        wo_copy(0, p).start()

    def all_of(ref, send, recv):
        return pltpu.make_async_remote_copy(ref, ref, send, recv, device_id=dev(1), device_id_type=MESH)

    all_ids = all_of(ids_all.at[0:7], ms_sem, mr_sem)
    all_gates = all_of(gate_all.at[0:7], gs_sem, gr_sem)
    all_ids.wait_recv()
    all_gates.wait_recv()

    lane = lax.broadcasted_iota(jnp.int32, (8, 128), 1)

    def compact(ref):
        out = []
        for m in range(4):
            a = ref[2 * m]
            b = pltpu.roll(ref[2 * m + 1], 64, 1)
            out += [a[:, :128], jnp.where(lane < 64, a[:, 128:], b[:, :128]), b[:, 128:]]
        return out

    id_blocks, gate_blocks = compact(ids_all), compact(gate_all)
    eid = lax.broadcasted_iota(jnp.int32, (8, 128), 0) + me * nexp
    imasks, gates = [], []
    for idb, gb in zip(id_blocks, gate_blocks):
        m = jnp.zeros((8, 128), jnp.int32)
        g = jnp.zeros((8, 128), F32)
        for k in range(8):
            hit = idb[k:k + 1, :] == eid
            m = jnp.where(hit, 1, m)
            g = jnp.where(hit, gb[k:k + 1, :], g)
        imasks.append(m)
        gates.append(g)
    masks = [m.astype(F32) for m in imasks]
    nb = len(masks)
    tri = jnp.where(lax.broadcasted_iota(jnp.int32, (128, 128), 0) < lax.broadcasted_iota(jnp.int32, (128, 128), 1),
                    1.0, 0.0).astype(BF)
    cums = jnp.dot(jnp.concatenate(masks, axis=0).astype(BF), tri, preferred_element_type=F32)
    carry = jnp.zeros((8, 1), F32)
    ranks = []
    for b in range(nb):
        ranks.append(cums[b * 8:b * 8 + 8, :] + carry)
        carry = carry + jnp.sum(masks[b], axis=1, keepdims=True)
    starts, seen = [], jnp.zeros((8, 128), jnp.int32)
    table = jnp.zeros((8, 128), jnp.int32)
    for g in range(8):
        b = 3 * (g // 2) + g % 2
        before = seen + jnp.where(lane < 64, imasks[b], 0) if g % 2 else seen
        off = jnp.sum(before, axis=1, keepdims=True)
        start16 = jnp.minimum(off >> 4, (cap - WIN) // 16)
        table = jnp.where(lane == g, start16, table)
        starts.append((start16 * 16).astype(F32))
        seen = seen + imasks[b]
        if g % 2:
            seen = seen + imasks[b + 1]
    start_v[...] = table
    st = pltpu.make_async_copy(start_v, start_s, st_sem)
    st.start()
    for b in range(nb):
        m = b // 3
        if b % 3 == 0:
            start = starts[2 * m]
        elif b % 3 == 1:
            start = jnp.where(lane < 64, starts[2 * m], starts[2 * m + 1])
        else:
            start = starts[2 * m + 1]
        keep = (masks[b] > 0.0) & (ranks[b] < float(cap))
        slot_buf[:, b * 128:(b + 1) * 128] = jnp.where(keep, ranks[b], -1.0)
        g1 = gates[b].astype(BF).astype(F32)
        rem1 = gates[b] - g1
        g2 = rem1.astype(BF).astype(F32)
        g3 = rem1 - g2
        zbuf[b, 0:8, :] = jnp.where(keep, ranks[b] - start, -1.0)
        zbuf[b, 8:16, :] = g1
        zbuf[b, 16:24, :] = g2
        zbuf[b, 24:32, :] = g3

    def build_p(e, _):
        row = slot_buf[pl.ds(e, 1), :]
        pos = lax.broadcasted_iota(jnp.int32, (cap, ntok), 0).astype(F32)
        pmat[pl.ds(pl.multiple_of(e * cap, 64), cap), :] = jnp.where(pos == row, 1.0, 0.0).astype(BF)
        return 0

    nwin = nexp * WIN

    def build_c(b, _):
        z = jnp.concatenate([zbuf[b], jnp.zeros((96, 128), F32)], axis=0)
        zt = jnp.transpose(z).astype(BF)
        ex = jnp.where(lax.broadcasted_iota(jnp.int32, (128, 4 * nwin), 0)
                       == lax.broadcasted_iota(jnp.int32, (128, 4 * nwin), 1) // WIN, 1.0, 0.0).astype(BF)
        y = jnp.dot(zt, ex, preferred_element_type=F32)
        wpos = lax.rem(lax.broadcasted_iota(jnp.int32, (128, nwin), 1), WIN).astype(F32)
        hit = y[:, :nwin] == wpos
        rows = pl.ds(pl.multiple_of(b * 128, 128), 128)
        for k in range(3):
            cmat[k, rows, :] = jnp.where(hit, y[:, (k + 1) * nwin:(k + 2) * nwin], 0.0).astype(BF)
        return 0

    def arrived(c):
        all_of(tok_all.at[c, 0:4 * tok_dev, :], as_sem, ar_sem.at[c, 0]).wait_recv()

    def first(c, part):
        experts = range(part * (nexp // 2), (part + 1) * (nexp // 2))
        wi_copy(c, part).wait()

        def dispatch(e):
            return jnp.dot(pmat[e * cap:(e + 1) * cap, :], tok_all[c], preferred_element_type=F32).astype(BF)

        def expand(e, rows):
            y = jnp.dot(rows, wi[part, e % nh], preferred_element_type=F32)
            for n in range(ff // wd):
                yn = y[:, n * wd:(n + 1) * wd]
                if c:
                    yn = yn + hacc[e * (ff // wd) + n]
                if c == nch - 1:
                    hbf[e * cap:(e + 1) * cap, n * wd:(n + 1) * wd] = gelu_tanh(yn).astype(BF)
                else:
                    hacc[e * (ff // wd) + n] = yn

        ready = None
        for e in experts:
            rows = dispatch(e)
            if ready is not None:
                expand(*ready)
            ready = (e, rows)
        expand(*ready)
        if c + 1 < nch:
            wi_copy(c + 1, part).start()

    lax.fori_loop(0, nexp, build_p, 0)
    near(0)
    send_own(2)
    lax.fori_loop(0, nb // 2, build_c, 0)
    near(1)
    send_own(3)
    lax.fori_loop(nb // 2, nb, build_c, 0)
    far(0)
    arrived(0)
    first(0, 0)
    first(0, 1)
    near(2)
    far(1)
    arrived(1)
    first(1, 0)
    near(3)
    first(1, 1)
    far(2)
    arrived(2)
    first(2, 0)
    far(3)
    first(2, 1)
    arrived(3)
    first(3, 0)
    first(3, 1)
    st.wait()

    def d2d_copy(c, q):
        k = c * 4 + q
        return pltpu.make_async_remote_copy(d2d_out.at[k], d2d_in.at[k], ds_sem, dr_sem.at[k],
                                            device_id=dev(1), device_id_type=MESH)

    def hop1(c, axis, k):
        recv = r1_sem.at[c, axis] if k else rf_sem.at[c]
        return pltpu.make_async_remote_copy(out1.at[c, axis, k], in1.at[c, axis, k], s1_sem, recv,
                                            device_id=dev(4 if axis else 2), device_id_type=MESH)

    def hop2(c, part):
        return pltpu.make_async_remote_copy(out2.at[c, part], in2.at[c, part], s2_sem, rf_sem.at[c],
                                            device_id=dev(2 if part else 4), device_id_type=MESH)

    def combine(r):
        g = gidx(r)
        parts = []
        for e in range(nexp):
            at = e * (cap // 16) + start_s[e, g]
            parts.append(obuf[pl.ds(at, WIN // 16)].reshape(WIN, wd))
        win = jnp.concatenate(parts, axis=0)
        rows = pl.ds(pl.multiple_of(g * tok_dev, 64), tok_dev)
        lhs = jnp.concatenate([cmat[k, rows, :] for k in range(3)], axis=0)
        y = jnp.dot(lhs, win, preferred_element_type=F32)
        return y[:tok_dev] + y[tok_dev:2 * tok_dev] + y[2 * tok_dev:]

    def relay(c):
        for part in range(2):
            hop1(c, part, 1).wait_recv()
            out2[c, part] = (kept[c, part] + in1[c, part, 1].astype(F32)).astype(BF)
            hop2(c, part).start()

    def finish(c):
        all_of(in1.at[c], s1_sem, rf_sem.at[c]).wait_recv()
        for part in range(2):
            own[c, part] = own[c, part] + in1[c, part, 0].astype(F32) + in2[c, part].astype(F32)
        out_copy(c).start()

    def second(c, _):
        for part in range(2):
            experts = range(part * (nexp // 2), (part + 1) * (nexp // 2))
            wo_copy(c, part).wait()
            for e in experts:
                y = jnp.dot(hbf[e * cap:(e + 1) * cap, :], wo[part, e % nh], preferred_element_type=F32).astype(BF)
                obuf[e * (cap // 16):(e + 1) * (cap // 16)] = y.reshape(cap // 16, 16, wd)

            @pl.when(c + 1 < nch)
            def _():
                wo_copy(c + 1, part).start()

        for pair in ((0, 1), (2, 3)):
            for q in pair:
                d2d_out[c * 4 + q] = combine(RETURN_ORDER[q] + 1).astype(BF)
            for q in pair:
                d2d_copy(c, q).start()
        for q in (0, 1):
            hacc[q] = combine(RETURN_ORDER[q])
        for q, r in enumerate(RETURN_ORDER):
            if q == 2:
                for k in (2, 3):
                    hacc[k] = combine(RETURN_ORDER[k])
            d2d_copy(c, q).wait_recv()
            y = hacc[q] + d2d_in[c * 4 + q].astype(F32)
            if r == 6:
                out1[c, 0, 1] = y[:half].astype(BF)
                out1[c, 1, 1] = y[half:].astype(BF)
                hop1(c, 0, 1).start()
                hop1(c, 1, 1).start()
            elif r == 2:
                out1[c, 0, 0] = y[:half].astype(BF)
                kept[c, 1] = y[half:]
                hop1(c, 0, 0).start()
            elif r == 4:
                out1[c, 1, 0] = y[half:].astype(BF)
                kept[c, 0] = y[:half]
                hop1(c, 1, 0).start()
            else:
                own[c, 0] = y[:half]
                own[c, 1] = y[half:]

        @pl.when(c > 0)
        def _():
            relay(c - 1)

        @pl.when(c > 1)
        def _():
            finish(c - 2)
        return 0

    lax.fori_loop(0, nch, second, 0)
    relay(nch - 1)
    finish(nch - 2)
    finish(nch - 1)

    all_ids.wait_send()
    all_gates.wait_send()
    all_of(tok_all.at[:, 0:7 * tok_dev, :], as_sem, ar_sem.at[0, 0]).wait_send()
    all_of(d2d_out, ds_sem, dr_sem.at[0]).wait_send()
    all_of(out1, s1_sem, rf_sem.at[0]).wait_send()
    all_of(out2, s2_sem, rf_sem.at[0]).wait_send()
    for c in range(nch):
        out_copy(c).wait()


def solution(mesh):
    group_size = mesh.shape['row'] * mesh.shape['col']

    def device_fn(tokens, expert_ids, gate_weights, w_in, w_out):
        tok_dev, width = tokens.shape
        top_k = expert_ids.shape[1]
        nexp, _, ff = w_in.shape
        cap = tok_dev * group_size * top_k // (nexp * group_size)
        ntok = tok_dev * group_size
        nch = 4
        wd = width // nch
        half = tok_dev // 2
        dma = pltpu.SemaphoreType.DMA
        cfg = (tok_dev, cap, nexp, nch, wd, ff)
        hb = pl.BlockSpec(memory_space=pl.ANY)
        mixed = pl.pallas_call(
            functools.partial(moe_kernel, cfg),
            out_shape=jax.ShapeDtypeStruct((2, half, width), F32),
            in_specs=[hb] * 5,
            out_specs=hb,
            scratch_shapes=[
                pltpu.VMEM((8, 8, 256), jnp.int32),
                pltpu.VMEM((8, 8, 256), F32),
                pltpu.VMEM((nch, ntok, wd), BF),
                pltpu.VMEM((nexp * cap, ntok), BF),
                pltpu.VMEM((3, ntok, nexp * WIN), BF),
                pltpu.VMEM((nexp * ff // wd, cap, wd), F32),
                pltpu.VMEM((nexp * cap, ff), BF),
                pltpu.VMEM((2, nexp // 2, wd, ff), BF),
                pltpu.VMEM((2, nexp // 2, ff, wd), BF),
                pltpu.VMEM((nexp * cap // 16, 16, wd), BF),
                pltpu.VMEM((nch * 4, tok_dev, wd), BF),
                pltpu.VMEM((nch * 4, tok_dev, wd), BF),
                pltpu.VMEM((nch, 2, 2, half, wd), BF),
                pltpu.VMEM((nch, 2, 2, half, wd), BF),
                pltpu.VMEM((nch, 2, half, wd), BF),
                pltpu.VMEM((nch, 2, half, wd), BF),
                pltpu.VMEM((nch, 2, half, wd), F32),
                pltpu.VMEM((nch, 2, half, wd), F32),
                pltpu.VMEM((8, tok_dev), jnp.int32),
                pltpu.VMEM((8, tok_dev), F32),
                pltpu.VMEM((8, ntok), F32),
                pltpu.VMEM((ntok // 128, 32, 128), F32),
                pltpu.VMEM((8, 128), jnp.int32),
                pltpu.SMEM((8, 128), jnp.int32),
                dma((nch,)), dma((2,)), dma((2,)), dma, dma, dma, dma, dma, dma((nch, 5)), dma, dma((nch * 4,)),
                dma, dma((nch, 2)), dma, dma((nch,)), dma, dma((nch,)), dma, dma,
            ],
            compiler_params=pltpu.CompilerParams(collective_id=0, has_side_effects=True, vmem_limit_bytes=67000000),
        )(expert_ids.T, gate_weights.T, tokens, w_in, w_out)
        return (tokens.astype(F32) + mixed.reshape(tok_dev, width)).astype(BF)

    token_spec = P(('data', 'row', 'col'), None)
    expert_spec = P(GRID_AXES, None, None)
    return jax.shard_map(device_fn, mesh=mesh, in_specs=(token_spec, token_spec, token_spec, expert_spec, expert_spec),
                         out_specs=token_spec, check_vma=False)
```
